256 devices in a mesh: north: 8 (over y_hi, x), east: 32 (over z, y_lo, core).
Axes of the slice: x: 4, y: 4 (y_hi: 2, y_lo: 2; y = y_hi * 2 + y_lo), z: 8, core: 2. Of those that a mesh axis runs over, the one named last changes fastest.
Arguments:
- pair_rows: bfloat16 [768, 768, 128], P('north', 'east'), may hold values from -6 to 6
- in_gain: float32 [128], replicated, may hold values from 0.25 to 1.75
- left_weight: bfloat16 [128, 128], replicated, may hold values from -0.5 to 0.5
- right_weight: bfloat16 [128, 128], replicated, may hold values from -0.5 to 0.5
- left_gate: bfloat16 [128, 128], replicated, may hold values from -0.5 to 0.5
- right_gate: bfloat16 [128, 128], replicated, may hold values from -0.5 to 0.5
- mid_gain: float32 [128], replicated, may hold values from 0.25 to 1.75
- out_weight: bfloat16 [128, 128], replicated, may hold values from -0.5 to 0.5
- out_gate: bfloat16 [128, 128], replicated, may hold values from -0.5 to 0.5
Outputs:
- pair_change: bfloat16 [768, 768, 128], P('north', 'east')
The draws below stay inside these ranges and needn't reach their ends.
All inputs are finite; a program needn't handle non-finite values.
Results may differ from the reference program's by a relative error of at most 0.012.
Values may be sent and summed in bfloat16 or wider, within the bound.
A program may use at most 128 MiB of HBM per device.

```python
import jax
import jax.numpy as jnp
from jax import lax

RESIDUES = 768
PAIR_WIDTH = 128
MIX_WIDTH = 128


def levels(stream_key, shape, split, smallest, top_value):
    level = 1.0
    for dim, shards_of in split:
        draws = jax.random.uniform(jax.random.fold_in(jax.random.fold_in(stream_key, 6), dim), (shards_of,), jnp.float32, smallest / len(split), top_value / len(split))
        level = level * jnp.repeat(jnp.exp(draws), shape[dim] // shards_of).reshape((-1,) + (1,) * (len(shape) - 1 - dim))
    return level


def scatter_about(own_key, dims, width, most, split=(), dtype=jnp.bfloat16):
    entries = jax.random.normal(own_key, dims, jnp.float32) * width
    if len(split) > 0:
        entries = levels(own_key, dims, split, -0.22, 0.18) * entries
    return jnp.clip(entries, min=-most, max=most).astype(dtype)


def setup_inputs(seed: int = 0) -> dict:
    key_list = jax.random.split(jax.random.key(seed), 10)
    return {
        "pair_rows": scatter_about(key_list[0], (RESIDUES, RESIDUES, PAIR_WIDTH), 1.0, 6.0, ((0, 8), (1, 32))),
        "in_gain": jnp.clip(1.0 + 0.15 * jax.random.normal(key_list[1], (PAIR_WIDTH,), jnp.float32), 0.25, 1.75),
        "left_weight": scatter_about(key_list[2], (PAIR_WIDTH, MIX_WIDTH), PAIR_WIDTH ** -0.5, 0.5),
        "right_weight": scatter_about(key_list[3], (PAIR_WIDTH, MIX_WIDTH), PAIR_WIDTH ** -0.5, 0.5),
        "left_gate": scatter_about(key_list[4], (PAIR_WIDTH, MIX_WIDTH), PAIR_WIDTH ** -0.5, 0.5),
        "right_gate": scatter_about(key_list[5], (PAIR_WIDTH, MIX_WIDTH), PAIR_WIDTH ** -0.5, 0.5),
        "mid_gain": jnp.clip(1.0 + 0.15 * jax.random.normal(key_list[6], (MIX_WIDTH,), jnp.float32), 0.25, 1.75),
        "out_weight": scatter_about(key_list[7], (MIX_WIDTH, PAIR_WIDTH), MIX_WIDTH ** -0.5, 0.5),
        "out_gate": scatter_about(key_list[8], (PAIR_WIDTH, PAIR_WIDTH), PAIR_WIDTH ** -0.5, 0.5),
    }


def scale_channels(values, channel_gain):
    centred = values - lax.optimization_barrier(jnp.mean(values, axis=-1, keepdims=True))
    return centred * lax.rsqrt(lax.optimization_barrier(jnp.mean(centred * centred, axis=-1, keepdims=True)) + 1e-05) * channel_gain

def both_factors(pair_in, in_gain, left_weight, right_weight, left_gate, right_gate):
    ready = scale_channels(pair_in.astype(jnp.float32), in_gain).astype(jnp.bfloat16)
    ready = lax.optimization_barrier(ready)
    left = jnp.einsum('ijc,cd->ijd', ready.astype(jnp.float32), left_weight.astype(jnp.float32))
    left = left * jax.nn.sigmoid(jnp.einsum('ijc,cd->ijd', ready.astype(jnp.float32), left_gate.astype(jnp.float32)))
    right = jnp.einsum('ijc,cd->ijd', ready.astype(jnp.float32), right_weight.astype(jnp.float32))
    right = right * jax.nn.sigmoid(jnp.einsum('ijc,cd->ijd', ready.astype(jnp.float32), right_gate.astype(jnp.float32)))
    return (ready, left.astype(jnp.bfloat16), right.astype(jnp.bfloat16))

def to_pair(mixed, ready, mid_gain, out_weight, out_gate):
    scaled = scale_channels(mixed.astype(jnp.float32), mid_gain).astype(jnp.bfloat16)
    scaled = lax.optimization_barrier(scaled)
    gate = jax.nn.sigmoid(jnp.einsum('ijc,cd->ijd', ready.astype(jnp.float32), out_gate.astype(jnp.float32)))
    return (jnp.einsum('ijd,dc->ijc', scaled.astype(jnp.float32), out_weight.astype(jnp.float32)) * gate).astype(jnp.bfloat16)

def reference(pair_rows, in_gain, left_weight, right_weight, left_gate, right_gate, mid_gain, out_weight, out_gate):
    ready, left, right = both_factors(pair_rows, in_gain, left_weight, right_weight, left_gate, right_gate)
    left, right = lax.optimization_barrier((left, right))

    def one_channel(pair_of):
        return (jnp.dot(pair_of[0].T, pair_of[1], preferred_element_type=jnp.float32) * RESIDUES ** (-0.5)).astype(jnp.bfloat16)
    mixed = jnp.moveaxis(lax.map(one_channel, (jnp.moveaxis(left, -1, 0), jnp.moveaxis(right, -1, 0))), 0, -1)
    mixed = lax.optimization_barrier(mixed)
    return to_pair(mixed, ready, mid_gain, out_weight, out_gate)
```

```python
import jax
import jax.numpy as jnp
from jax import lax
from jax.experimental import pallas as pl
from jax.experimental.pallas import tpu as pltpu
from jax.sharding import PartitionSpec as P

MESH = pl.DeviceIdType.MESH
F32, BF16 = jnp.float32, jnp.bfloat16

RES, WIDTH = 768, 128
NORTH, EAST, CHIPS = 8, 32, 16
KB, IB = RES // NORTH, RES // EAST
ROWS = KB * IB
GROUP = WIDTH // NORTH
SPAN = 4 * KB
STEPS = ROWS // SPAN
HALF = RES // 2


def turn(values, amount):
    amount = amount % SPAN
    return values if amount == 0 else pltpu.roll(values, amount, axis=1)


def regroup(parts):
    lane = lax.broadcasted_iota(jnp.int32, parts[0].shape, 1)
    out = []
    for b in range(4):
        row = turn(parts[0], -KB * b)
        for a in range(1, 4):
            row = jnp.where(lane >= KB * a, turn(parts[a], KB * (a - b)), row)
        out.append(row)
    return out


def nt(a, b):
    return lax.dot_general(a, b, (((1,), (1,)), ((), ())), preferred_element_type=F32)


def kernel(
    x_ref, in_gain, lw, rw, lg, rg, mid_gain, ow, og, out_ref,
    flat, ready, wt, send1, got1, mid, send2, left, right, sums, got3, send4, got4, gate, gain_col,
    s1, r1, s2l, r2l, s2r, r2r, sf, rf, s3, r3, s4, r4,
):
    n = lax.axis_index("north")
    e = lax.axis_index("east")
    zy, c = e // 2, lax.rem(e, 2)
    half = zy // 8

    def remote(src, dst, ssem, rsem, where):
        return pltpu.make_async_remote_copy(
            src_ref=src, dst_ref=dst, send_sem=ssem, recv_sem=rsem,
            device_id=where, device_id_type=MESH,
        )

    barrier = pltpu.get_barrier_semaphore()
    for s in range(1, NORTH):
        pl.semaphore_signal(
            barrier, inc=1, device_id={"north": lax.rem(n + s, NORTH)}, device_id_type=MESH
        )
    for s in range(1, EAST):
        pl.semaphore_signal(
            barrier, inc=1, device_id={"east": lax.rem(e + s, EAST)}, device_id_type=MESH
        )

    @pl.loop(0, 4)
    def _(b):
        rows = pl.ds(b * (ROWS // 4), ROWS // 4)
        v = x_ref[rows, :].astype(F32)
        v = v - jnp.mean(v, axis=-1, keepdims=True)
        v = v * lax.rsqrt(jnp.mean(v * v, axis=-1, keepdims=True) + 1e-05) * in_gain[...]
        flat[rows, :] = v

    for i in range(IB):
        ready[i * KB : (i + 1) * KB, :] = flat[pl.ds(i, KB, stride=IB), :].astype(BF16)

    for p, w in enumerate((lw, lg, rw, rg)):
        wt[p * WIDTH : (p + 1) * WIDTH, :] = w[...].astype(F32).T.astype(BF16)
    gain_col[...] = jnp.broadcast_to(mid_gain[...], (WIDTH, WIDTH)).T

    hop1 = [[], []]
    for a in range(2):

        @pl.loop(0, STEPS)
        def _(g, a=a):
            cols = pl.ds(pl.multiple_of(g * SPAN, SPAN), SPAN)
            both = nt(wt[2 * a * WIDTH : 2 * (a + 1) * WIDTH, :], ready[cols, :])
            send1[a, :, cols] = (both[:WIDTH] * jax.nn.sigmoid(both[WIDTH:])).astype(BF16)

        if a == 0:
            pl.semaphore_wait(barrier, NORTH + EAST - 2)
        for s in range(1, NORTH):
            to = lax.rem(n + s, NORTH)
            copy = remote(
                send1.at[a, pl.ds(pl.multiple_of(to * GROUP, GROUP), GROUP), :],
                got1.at[a, n],
                s1.at[a, s], r1.at[a, s], {"north": to},
            )
            copy.start()
            hop1[a].append(copy)
        got1[a, n] = send1[a, pl.ds(pl.multiple_of(n * GROUP, GROUP), GROUP), :]

    def spread(a):
        @pl.loop(0, STEPS)
        def _(g):
            cols = pl.ds(pl.multiple_of(g * SPAN, SPAN), SPAN)
            for h in range(2):
                parts = [got1[a, 4 * h + q, :, cols].astype(F32) for q in range(4)]
                for b, row in enumerate(regroup(parts)):
                    for u in range(3):
                        mid[3 * h + u, pl.ds(4 * g + b, GROUP, stride=IB), :] = row[
                            :, u * 128 : (u + 1) * 128
                        ]

        @pl.loop(0, CHIPS)
        def _(d):
            for t in range(6):
                send2[a, d, :, t * 128 : (t + 1) * 128] = mid[
                    t, pl.ds(pl.multiple_of(d * IB, IB), IB), :
                ].astype(BF16)

    for copy in hop1[0]:
        copy.wait_recv()
    spread(0)
    lrow = pl.multiple_of((lax.rem(zy, 8) * 2 + c) * IB, IB)
    lsrc = lax.rem(zy, 8) * 2 + c
    hop2l = []
    for s in range(1, CHIPS):
        to = lax.rem(zy + s, CHIPS)
        copy = remote(
            send2.at[0, to], left.at[pl.ds(lrow, IB), :],
            s2l.at[s], r2l.at[lsrc], {"east": to * 2 + half},
        )
        copy.start()
        hop2l.append(copy)

    own_l = remote(
        send2.at[0, zy], left.at[pl.ds(lrow, IB), :], s2l.at[0], r2l.at[lsrc], {"east": zy * 2 + half}
    )

    @pl.when(c != half)
    def _():
        own_l.start()

    @pl.when(c == half)
    def _():
        left[pl.ds(lrow, IB), :] = send2[0, zy]

    for copy in hop1[1]:
        copy.wait_recv()
    spread(1)
    hop2r = []
    rrow = pl.multiple_of(e * IB, IB)
    partner = {"east": zy * 2 + 1 - c}
    for s in range(1, CHIPS):
        to = lax.rem(zy + s, CHIPS)
        copy = remote(
            send2.at[1, to], right.at[pl.ds(rrow, IB), :],
            s2r.at[s], r2r.at[s], {"east": to * 2 + c},
        )
        copy.start()
        hop2r.append(copy)
    shared = [
        remote(send2.at[1, zy], right.at[pl.ds(rrow, IB), :], sf.at[0], rf.at[0], partner)
    ]
    shared[0].start()
    right[pl.ds(rrow, IB), :] = send2[1, zy]

    @pl.loop(0, STEPS)
    def _(g):
        rows = pl.ds(pl.multiple_of(g * SPAN, SPAN), SPAN)
        gate[rows, :] = jax.nn.sigmoid(
            jnp.dot(ready[rows, :], og[...], preferred_element_type=F32)
        )

    for s in range(1, CHIPS):
        hop2r[s - 1].wait_recv()
        origin = lax.rem(zy + CHIPS - s, CHIPS) * 2 + c
        rows = pl.ds(pl.multiple_of(origin * IB, IB), IB)
        copy = remote(right.at[rows, :], right.at[rows, :], sf.at[s], rf.at[s], partner)
        copy.start()
        shared.append(copy)

    for p in range(CHIPS):

        @pl.when(jnp.logical_not((zy // 8 == c) & (lsrc == p)))
        def _(p=p):
            remote(
                send2.at[0, 0], left.at[pl.ds(p * IB, IB), :], s2l.at[0], r2l.at[p], partner
            ).wait_recv()

    for copy in shared:
        copy.wait_recv()

    hop3 = []
    quarter = RES // 4
    for t in range(4):
        at = lax.rem(zy // 4 + t, 4)
        rows = pl.ds(pl.multiple_of(at * quarter, quarter), quarter)
        sums[rows, :] = (nt(right[rows, :], left[...]) * RES ** (-0.5)).astype(BF16)
        for p in range(EAST // 4):
            to = at * (EAST // 4) + p
            block = sums.at[pl.ds(pl.multiple_of(to * IB, IB), IB), :]
            copy = remote(
                block, got3.at[zy, :, pl.ds(pl.multiple_of(c * HALF, HALF), HALF)],
                s3.at[t * (EAST // 4) + p], r3.at[e], {"east": to},
            )
            hop3.append((copy, to))

            @pl.when(to != e)
            def _(copy=copy):
                copy.start()

    mine = sums[pl.ds(pl.multiple_of(e * IB, IB), IB), :]

    @pl.when(c == 0)
    def _():
        got3[zy, :, :HALF] = mine

    @pl.when(c == 1)
    def _():
        got3[zy, :, HALF:] = mine

    hop4 = []
    for h in range(2):
        for p in range(CHIPS):
            @pl.when(jnp.logical_not((zy == p) & (c == h)))
            def _(p=p, h=h):
                remote(
                    sums.at[pl.ds(0, IB), :], got3.at[p, :, pl.ds(h * HALF, HALF)],
                    s3.at[0], r3.at[2 * p + h], partner,
                ).wait_recv()

        @pl.loop(0, CHIPS)
        def _(d, h=h):
            for u in range(3):
                t = 3 * h + u
                mid[t, pl.ds(pl.multiple_of(d * IB, IB), IB), :] = got3[
                    d, :, t * 128 : (t + 1) * 128
                ].astype(F32)

        @pl.loop(0, STEPS)
        def _(g, h=h):
            cols = pl.ds(pl.multiple_of(g * SPAN, SPAN), SPAN)
            parts = [
                jnp.concatenate(
                    [mid[3 * h + u, pl.ds(4 * g + b, GROUP, stride=IB), :] for u in range(3)], axis=1
                )
                for b in range(4)
            ]
            for q, row in enumerate(regroup(parts)):
                send4[4 * h + q, :, cols] = row.astype(BF16)

        for q in range(4):
            to = 4 * h + q
            copy = remote(
                send4.at[to], got4.at[pl.ds(pl.multiple_of(n * GROUP, GROUP), GROUP), :],
                s4.at[to], r4.at[n], {"north": to},
            )
            hop4.append(copy)

            @pl.when(to != n)
            def _(copy=copy):
                copy.start()

    got4[pl.ds(pl.multiple_of(n * GROUP, GROUP), GROUP), :] = send4[n]
    for p in range(NORTH):

        @pl.when(p != n)
        def _(p=p):
            remote(
                send4.at[0], got4.at[pl.ds(p * GROUP, GROUP), :], s4.at[0], r4.at[p], partner
            ).wait_recv()

    @pl.loop(0, STEPS)
    def _(g):
        cols = pl.ds(pl.multiple_of(g * SPAN, SPAN), SPAN)
        v = got4[:, cols].astype(F32)
        v = v - jnp.mean(v, axis=0, keepdims=True)
        v = v * lax.rsqrt(jnp.mean(v * v, axis=0, keepdims=True) + 1e-05)
        gains = jnp.concatenate([gain_col[...]] * 3, axis=1)
        v = (v * gains).astype(BF16)
        y = lax.dot_general(v, ow[...], (((0,), (0,)), ((), ())), preferred_element_type=F32)
        y = y * gate[cols, :]
        for b in range(4):
            flat[pl.ds(4 * g + b, KB, stride=IB), :] = y[b * KB : (b + 1) * KB]

    @pl.loop(0, 4)
    def _(b):
        rows = pl.ds(b * (ROWS // 4), ROWS // 4)
        out_ref[rows, :] = flat[rows, :].astype(BF16)

    for copy in hop1[0] + hop1[1] + hop2l + hop2r + shared:
        copy.wait_send()

    @pl.when(c != half)
    def _():
        own_l.wait_send()

    for copy, to in hop3:

        @pl.when(to != e)
        def _(copy=copy):
            copy.wait_send()

    for to, copy in enumerate(hop4):

        @pl.when(to != n)
        def _(copy=copy):
            copy.wait_send()


def body(pair_rows, in_gain, left_weight, right_weight, left_gate, right_gate, mid_gain, out_weight, out_gate):
    dma = pltpu.SemaphoreType.DMA
    vmem = pltpu.VMEM
    out = pl.pallas_call(
        kernel,
        out_shape=jax.ShapeDtypeStruct((ROWS, WIDTH), BF16),
        in_specs=[pl.BlockSpec(memory_space=vmem)] * 9,
        out_specs=pl.BlockSpec(memory_space=vmem),
        scratch_shapes=[
            vmem((ROWS, WIDTH), F32),
            vmem((ROWS, WIDTH), BF16),
            vmem((4 * WIDTH, WIDTH), BF16),
            vmem((2, WIDTH, ROWS), BF16),
            vmem((2, NORTH, GROUP, ROWS), BF16),
            vmem((6, GROUP * IB, 128), F32),
            vmem((2, CHIPS, IB, RES), BF16),
            vmem((HALF, RES), BF16),
            vmem((RES, RES), BF16),
            vmem((RES, HALF), BF16),
            vmem((CHIPS, IB, RES), BF16),
            vmem((NORTH, GROUP, ROWS), BF16),
            vmem((WIDTH, ROWS), BF16),
            vmem((ROWS, WIDTH), F32),
            vmem((WIDTH, WIDTH), F32),
            dma((2, NORTH)), dma((2, NORTH)),
            dma((CHIPS,)), dma((CHIPS,)),
            dma((CHIPS,)), dma((CHIPS,)),
            dma((CHIPS,)), dma((CHIPS,)),
            dma((EAST,)), dma((EAST,)),
            dma((NORTH,)), dma((NORTH,)),
        ],
        compiler_params=pltpu.CompilerParams(
            collective_id=0, has_side_effects=True, vmem_limit_bytes=60 * 2**20
        ),
        name="triangle",
    )(
        pair_rows.reshape(ROWS, WIDTH), in_gain.reshape(1, WIDTH), left_weight, right_weight,
        left_gate, right_gate, mid_gain.reshape(1, WIDTH), out_weight, out_gate,
    )
    return out.reshape(KB, IB, WIDTH)


def solution(mesh):
    placed = (P("north", "east", None), P(), P(), P(), P(), P(), P(), P(), P())
    return jax.shard_map(
        body, mesh=mesh, in_specs=placed, out_specs=P("north", "east", None), check_vma=False
    )
```

```python
import jax
import jax.numpy as jnp
from jax import lax
from jax.experimental import pallas as pl
from jax.experimental.pallas import tpu as pltpu
from jax.sharding import PartitionSpec as P

MESH = pl.DeviceIdType.MESH
F32, BF16 = jnp.float32, jnp.bfloat16

RES, WIDTH = 768, 128
NORTH, EAST, PLANE, DEPTH = 8, 32, 16, 8
KB, IB = RES // NORTH, RES // EAST
ROWS = KB * IB
WAVES, WI = 3, 8
LANES = WI * KB
SPAN = 4 * KB
HALF = RES // 2
PIECE = 2 * WI
SIDE = DEPTH * PIECE

STANDS = [y * 48 + c * 24 + w * WI for c in range(2) for w in range(WAVES) for y in range(2)]


def turn(values, amount):
    amount = amount % SPAN
    return values if amount == 0 else pltpu.roll(values, amount, axis=1)


def regroup(parts):
    lane = lax.broadcasted_iota(jnp.int32, parts[0].shape, 1)
    out = []
    for b in range(4):
        row = turn(parts[0], -KB * b)
        for a in range(1, 4):
            row = jnp.where(lane >= KB * a, turn(parts[a], KB * (a - b)), row)
        out.append(row)
    return out


def nt(a, b):
    return lax.dot_general(a, b, (((1,), (1,)), ((), ())), preferred_element_type=F32)


def remote(src, dst, ssem, rsem, where):
    return pltpu.make_async_remote_copy(
        src_ref=src, dst_ref=dst, send_sem=ssem, recv_sem=rsem,
        device_id=where, device_id_type=MESH,
    )


def kernel(
    x_ref, in_gain, lw, rw, lg, rg, mid_gain, ow, og, out_ref,
    flat, ready, wt, send1, got1, mid, send2, left, right, sums, got3, send4, got4, gate, gain_col,
    s1, r1, s2, r2, sf, rf, s3, r3, s4, r4,
):
    n = lax.axis_index("north")
    e = lax.axis_index("east")
    z, y, c = e // 4, lax.rem(e // 2, 2), lax.rem(e, 2)
    plane = n * 2 + y
    half = z // 4

    def on_plane(p):
        return (p // 2, (z * 2 + lax.rem(p, 2)) * 2 + c)

    def on_line(to_z, to_c):
        return (n, (to_z * 2 + y) * 2 + to_c)

    partner = on_line(z, 1 - c)

    with jax.named_scope("signal"):
        barrier = pltpu.get_barrier_semaphore()
        for s in range(1, 16):
            t = lax.rem(z * 2 + c + s, 16)
            for where in (on_plane(lax.rem(plane + s, PLANE)), on_line(t // 2, lax.rem(t, 2))):
                pl.semaphore_signal(barrier, inc=1, device_id=where, device_id_type=MESH)

    with jax.named_scope("norm"):

        @pl.loop(0, 4)
        def _(b):
            rows = pl.ds(b * (ROWS // 4), ROWS // 4)
            v = x_ref[rows, :].astype(F32)
            v = v - jnp.mean(v, axis=-1, keepdims=True)
            v = v * lax.rsqrt(jnp.mean(v * v, axis=-1, keepdims=True) + 1e-05) * in_gain[...]
            flat[rows, :] = v

    with jax.named_scope("perm"):
        for i in range(IB):
            line = [flat[pl.ds(k * IB + i, WI, stride=IB), :] for k in STANDS]
            ready[i * KB : (i + 1) * KB, :] = jnp.concatenate(line, axis=0).astype(BF16)
        for p, w in enumerate((lw, lg, rw, rg)):
            wt[p * WIDTH : (p + 1) * WIDTH, :] = w[...].astype(F32).T.astype(BF16)
        gain_col[...] = jnp.broadcast_to(mid_gain[...], (WIDTH, WIDTH)).T

    def project(a, w):
        for g in range(2):
            rows = ready[w * LANES + g * SPAN : w * LANES + (g + 1) * SPAN, :]
            both = nt(wt[2 * a * WIDTH : 2 * (a + 1) * WIDTH, :], rows)
            both = both[:WIDTH] * jax.nn.sigmoid(both[WIDTH:])
            send1[a, w, :, :, g * SPAN : (g + 1) * SPAN] = both.reshape(PLANE, 8, SPAN).astype(BF16)

    def across(a, w):
        for s in range(1, PLANE):
            to = lax.rem(plane + s, PLANE)
            remote(
                send1.at[a, w, to], got1.at[a, w, plane], s1.at[a, w], r1.at[a, w], on_plane(to)
            ).start()
        got1[a, w, plane] = send1[a, w, plane]

    def spread(a, w):
        rest = got1.at[a, w, pl.ds(0, PLANE - 1)]
        with jax.named_scope(f"wait1#{a}{w}"):
            remote(rest, rest, s1.at[a, w], r1.at[a, w], partner).wait_recv()
        with jax.named_scope(f"spread#{a}{w}"):
            for yy in range(2):
                for g in range(2):
                    for h in range(2):
                        parts = [
                            got1[a, w, (4 * h + q) * 2 + yy, :, g * SPAN : (g + 1) * SPAN].astype(F32)
                            for q in range(4)
                        ]
                        for b, row in enumerate(regroup(parts)):
                            for u in range(3):
                                at = pl.ds(yy * WI + 4 * g + b, DEPTH, stride=PIECE)
                                mid[3 * h + u, at, :] = row[:, u * 128 : (u + 1) * 128]
            for d in range(DEPTH):
                for t in range(6):
                    send2[a, w, d, :, t * 128 : (t + 1) * 128] = mid[
                        t, d * PIECE : (d + 1) * PIECE, :
                    ].astype(BF16)

    def left_at(w):
        return pl.ds(pl.multiple_of(lax.rem(z, 4) * KB + c * 48 + w * PIECE, PIECE), PIECE)

    right_at = pl.ds(pl.multiple_of(c * SIDE + z * PIECE, PIECE), PIECE)

    def along(a, w):
        for s in (1, 7, 2, 6, 3, 5, 4):
            to = lax.rem(z + s, DEPTH)
            if a == 0:
                dst, where = left.at[left_at(w), :], on_line(to, half)
            else:
                dst, where = right.at[w, right_at, :], on_line(to, c)
            remote(send2.at[a, w, to], dst, s2.at[a, w], r2.at[a, w], where).start()
        if a == 1:
            right[w, right_at, :] = send2[1, w, z]
        else:

            @pl.when(c == half)
            def _():
                left[left_at(w), :] = send2[0, w, z]

            @pl.when(c != half)
            def _():
                remote(
                    send2.at[0, w, z], left.at[left_at(w), :], s2.at[0, w], r2.at[0, w], partner
                ).start()

    with jax.named_scope("proj"):
        for a in range(2):
            for w in range(WAVES):
                project(a, w)
                if a == 0 and w == 0:
                    with jax.named_scope("barrier"):
                        pl.semaphore_wait(barrier, 30)
                across(a, w)

    for a in range(2):
        for w in range(WAVES):
            spread(a, w)
            with jax.named_scope(f"along#{a}{w}"):
                along(a, w)

    with jax.named_scope("gate"):

        @pl.loop(0, ROWS // SPAN)
        def _(g):
            rows = pl.ds(pl.multiple_of(g * SPAN, SPAN), SPAN)
            gate[rows, :] = jax.nn.sigmoid(
                jnp.dot(ready[rows, :], og[...], preferred_element_type=F32)
            )

    def share(w):
        mine = right.at[w, pl.ds(pl.multiple_of(c * SIDE, SIDE), SIDE), :]
        return remote(mine, mine, sf.at[w], rf.at[w], partner)

    def multiply(w):
        with jax.named_scope(f"wait2#{w}"):
            some = send2.at[1, w, pl.ds(0, DEPTH - 1)]
            remote(some, some, s2.at[1, w], r2.at[1, w], partner).wait_recv()
            share(w).start()
        if w == 0:
            with jax.named_scope("waitleft"):
                for ww in range(WAVES):
                    for count in (DEPTH, DEPTH - 1):

                        @pl.when((c == half) if count == DEPTH - 1 else (c != half))
                        def _(ww=ww, count=count):
                            some = send2.at[0, ww, pl.ds(0, count)]
                            remote(some, some, s2.at[0, ww], r2.at[0, ww], partner).wait_recv()

        with jax.named_scope(f"waitshare#{w}"):
            share(w).wait_recv()
        with jax.named_scope(f"mm#{w}"):
            sums[w] = (nt(right[w], left[...]) * RES ** (-0.5)).astype(BF16)
            for s in range(1, 16):
                t = lax.rem(z * 2 + c + s, 16)
                to_z, to_c = t // 2, lax.rem(t, 2)
                at = pl.ds(pl.multiple_of(to_c * SIDE + to_z * PIECE, PIECE), PIECE)
                remote(
                    sums.at[w, at, :],
                    got3.at[w, z, :, pl.ds(pl.multiple_of(c * HALF, HALF), HALF)],
                    s3.at[w], r3.at[w], on_line(to_z, to_c),
                ).start()
            mine = sums[w, right_at, :]

            @pl.when(c == 0)
            def _():
                got3[w, z, :, :HALF] = mine

            @pl.when(c == 1)
            def _():
                got3[w, z, :, HALF:] = mine

    for w in range(WAVES):
        multiply(w)

    def gather(w):
        with jax.named_scope(f"wait3#{w}"):
            some = sums.at[w, pl.ds(0, 15 * PIECE), :]
            remote(some, some, s3.at[w], r3.at[w], partner).wait_recv()
        with jax.named_scope(f"gather#{w}"):
            for d in range(DEPTH):
                for t in range(6):
                    mid[t, d * PIECE : (d + 1) * PIECE, :] = got3[
                        w, d, :, t * 128 : (t + 1) * 128
                    ].astype(F32)
            for yy in range(2):
                for g in range(2):
                    for h in range(2):
                        parts = [
                            jnp.concatenate(
                                [
                                    mid[3 * h + u, pl.ds(yy * WI + 4 * g + b, DEPTH, stride=PIECE), :]
                                    for u in range(3)
                                ],
                                axis=1,
                            )
                            for b in range(4)
                        ]
                        for q, row in enumerate(regroup(parts)):
                            send4[w, (4 * h + q) * 2 + yy, :, g * SPAN : (g + 1) * SPAN] = row.astype(BF16)
            for s in range(1, PLANE):
                to = lax.rem(plane + s, PLANE)
                remote(send4.at[w, to], got4.at[w, plane], s4.at[w], r4.at[w], on_plane(to)).start()
            got4[w, plane] = send4[w, plane]

    def finish(w):
        with jax.named_scope(f"wait4#{w}"):
            rest = got4.at[w, pl.ds(0, PLANE - 1)]
            remote(rest, rest, s4.at[w], r4.at[w], partner).wait_recv()
        with jax.named_scope(f"finish#{w}"):
            gains = jnp.concatenate([gain_col[...]] * 3, axis=1)
            for g in range(2):
                v = got4[w, :, :, g * SPAN : (g + 1) * SPAN].astype(F32).reshape(WIDTH, SPAN)
                v = v - jnp.mean(v, axis=0, keepdims=True)
                v = v * lax.rsqrt(jnp.mean(v * v, axis=0, keepdims=True) + 1e-05)
                v = (v * gains).astype(BF16)
                out = lax.dot_general(v, ow[...], (((0,), (0,)), ((), ())), preferred_element_type=F32)
                out = out * gate[w * LANES + g * SPAN : w * LANES + (g + 1) * SPAN, :]
                for b in range(4):
                    for p, i in enumerate(STANDS):
                        flat[pl.ds(i * IB + w * WI + 4 * g + b, WI, stride=IB), :] = out[
                            b * KB + p * WI : b * KB + (p + 1) * WI
                        ]

    gather(0)
    gather(1)
    finish(0)
    gather(2)
    finish(1)
    finish(2)

    with jax.named_scope("store"):

        @pl.loop(0, 4)
        def _(b):
            rows = pl.ds(b * (ROWS // 4), ROWS // 4)
            out_ref[rows, :] = flat[rows, :].astype(BF16)

    def sent(ref, sem):
        remote(ref, ref, sem, r4.at[0], partner).wait_send()

    with jax.named_scope("sent"):
        for w in range(WAVES):
            for a in range(2):
                sent(send1.at[a, w, pl.ds(0, PLANE - 1)], s1.at[a, w])
            sent(send2.at[1, w, pl.ds(0, DEPTH - 1)], s2.at[1, w])
            for count in (DEPTH, DEPTH - 1):

                @pl.when((c == half) if count == DEPTH - 1 else (c != half))
                def _(w=w, count=count):
                    sent(send2.at[0, w, pl.ds(0, count)], s2.at[0, w])

            share(w).wait_send()
            sent(sums.at[w, pl.ds(0, 15 * PIECE), :], s3.at[w])
            sent(send4.at[w, pl.ds(0, PLANE - 1)], s4.at[w])


def body(pair_rows, in_gain, left_weight, right_weight, left_gate, right_gate, mid_gain, out_weight, out_gate):
    dma = pltpu.SemaphoreType.DMA
    vmem = pltpu.VMEM
    out = pl.pallas_call(
        kernel,
        out_shape=jax.ShapeDtypeStruct((ROWS, WIDTH), BF16),
        in_specs=[pl.BlockSpec(memory_space=vmem)] * 9,
        out_specs=pl.BlockSpec(memory_space=vmem),
        scratch_shapes=[
            vmem((ROWS, WIDTH), F32),
            vmem((ROWS, WIDTH), BF16),
            vmem((4 * WIDTH, WIDTH), BF16),
            vmem((2, WAVES, PLANE, 8, LANES), BF16),
            vmem((2, WAVES, PLANE, 8, LANES), BF16),
            vmem((6, DEPTH * PIECE, 128), F32),
            vmem((2, WAVES, DEPTH, PIECE, RES), BF16),
            vmem((HALF, RES), BF16),
            vmem((WAVES, 2 * SIDE, RES), BF16),
            vmem((WAVES, 2 * SIDE, HALF), BF16),
            vmem((WAVES, DEPTH, PIECE, RES), BF16),
            vmem((WAVES, PLANE, 8, LANES), BF16),
            vmem((WAVES, PLANE, 8, LANES), BF16),
            vmem((ROWS, WIDTH), F32),
            vmem((WIDTH, WIDTH), F32),
            dma((2, WAVES)), dma((2, WAVES)),
            dma((2, WAVES)), dma((2, WAVES)),
            dma((WAVES,)), dma((WAVES,)),
            dma((WAVES,)), dma((WAVES,)),
            dma((WAVES,)), dma((WAVES,)),
        ],
        compiler_params=pltpu.CompilerParams(
            collective_id=0, has_side_effects=True, vmem_limit_bytes=60 * 2**20
        ),
        name="triangle",
    )(
        pair_rows.reshape(ROWS, WIDTH), in_gain.reshape(1, WIDTH), left_weight, right_weight,
        left_gate, right_gate, mid_gain.reshape(1, WIDTH), out_weight, out_gate,
    )
    return out.reshape(KB, IB, WIDTH)


def solution(mesh):
    placed = (P("north", "east", None), P(), P(), P(), P(), P(), P(), P(), P())
    return jax.shard_map(
        body, mesh=mesh, in_specs=placed, out_specs=P("north", "east", None), check_vma=False
    )
```

```python
import jax
import jax.numpy as jnp
from jax import lax
from jax.experimental import pallas as pl
from jax.experimental.pallas import tpu as pltpu
from jax.sharding import PartitionSpec as P

MESH = pl.DeviceIdType.MESH
F32, BF16 = jnp.float32, jnp.bfloat16

RES, WIDTH = 768, 128
NORTH, EAST, PLANE, DEPTH = 8, 32, 16, 8
KB, IB = RES // NORTH, RES // EAST
ROWS = KB * IB
WAVES, WI = 3, 8
LANES = WI * KB
SPAN = 4 * KB
HALF = RES // 2
PIECE = 2 * WI
SIDE = DEPTH * PIECE

STANDS = [y * 48 + c * 24 + w * WI for c in range(2) for w in range(WAVES) for y in range(2)]


def turn(values, amount):
    amount = amount % SPAN
    return values if amount == 0 else pltpu.roll(values, amount, axis=1)


def regroup(parts):
    lane = lax.broadcasted_iota(jnp.int32, parts[0].shape, 1)
    out = []
    for b in range(4):
        row = turn(parts[0], -KB * b)
        for a in range(1, 4):
            row = jnp.where(lane >= KB * a, turn(parts[a], KB * (a - b)), row)
        out.append(row)
    return out


def nt(a, b):
    return lax.dot_general(a, b, (((1,), (1,)), ((), ())), preferred_element_type=F32)


def remote(src, dst, ssem, rsem, where):
    return pltpu.make_async_remote_copy(
        src_ref=src, dst_ref=dst, send_sem=ssem, recv_sem=rsem,
        device_id=where, device_id_type=MESH,
    )


def kernel(
    x_hbm, in_gain_hbm, lw_hbm, rw_hbm, lg_hbm, rg_hbm, mid_gain_hbm, ow_hbm, og_hbm, out_ref,
    x, in_gain, mid_gain, weights, turned, flat, ready, wt, send1, got1, mid, lines, send2, got2,
    left, right, sums, got3, send4, got4, gate, gain_col,
    xs, gs, wsem, s1, r1, s2, r2, sf, rf, s3, r3, s4, r4,
):
    n = lax.axis_index("north")
    e = lax.axis_index("east")
    z, y, c = e // 4, lax.rem(e // 2, 2), lax.rem(e, 2)
    plane = n * 2 + y
    half = z // 4

    def on_plane(p):
        return (p // 2, (z * 2 + lax.rem(p, 2)) * 2 + c)

    def on_line(to_z, to_c):
        return (n, (to_z * 2 + y) * 2 + to_c)

    partner = on_line(z, 1 - c)

    fetch_x = [
        pltpu.make_async_copy(x_hbm.at[:, pl.ds(w * WI, WI), :], x.at[w], xs.at[w])
        for w in range(WAVES)
    ]
    fetch_w = [
        pltpu.make_async_copy(ref, weights.at[p], wsem.at[p])
        for p, ref in enumerate((lw_hbm, lg_hbm, rw_hbm, rg_hbm, ow_hbm, og_hbm))
    ]
    fetch_g = [
        pltpu.make_async_copy(in_gain_hbm, in_gain, gs.at[0]),
        pltpu.make_async_copy(mid_gain_hbm, mid_gain, gs.at[1]),
    ]
    for copy in [fetch_x[0], fetch_g[0], *fetch_w[:2], *fetch_x[1:], *fetch_w[2:], fetch_g[1]]:
        copy.start()

    with jax.named_scope("signal"):
        barrier = pltpu.get_barrier_semaphore()
        for s in range(1, 16):
            t = lax.rem(z * 2 + c + s, 16)
            for where in (on_plane(lax.rem(plane + s, PLANE)), on_line(t // 2, lax.rem(t, 2))):
                pl.semaphore_signal(barrier, inc=1, device_id=where, device_id_type=MESH)

    def normalize(w):
        with jax.named_scope(f"norm#{w}"):
            fetch_x[w].wait()
            if w == 0:
                fetch_g[0].wait()
            v = x[w].astype(F32).reshape(LANES, WIDTH)
            v = v - jnp.mean(v, axis=-1, keepdims=True)
            v = v * lax.rsqrt(jnp.mean(v * v, axis=-1, keepdims=True) + 1e-05) * in_gain[...]
            flat[w * LANES : (w + 1) * LANES, :] = v
            for i in range(WI):
                line = [flat[pl.ds(w * LANES + k * WI + i, WI, stride=WI), :] for k in STANDS]
                at = (w * WI + i) * KB
                ready[at : at + KB, :] = jnp.concatenate(line, axis=0).astype(BF16)

    def orient(a):
        for p in range(2 * a, 2 * a + 2):
            fetch_w[p].wait()
            turned[p] = weights[p].astype(F32).T
            for to in range(DEPTH):
                at = p * WIDTH + to * PLANE
                wt[at : at + PLANE, :] = turned[p, pl.ds(to, PLANE, stride=DEPTH), :].astype(BF16)

    def project(a, w):
        with jax.named_scope(f"project#{a}{w}"):
            for g in range(2):
                rows = ready[w * LANES + g * SPAN : w * LANES + (g + 1) * SPAN, :]
                both = nt(wt[2 * a * WIDTH : 2 * (a + 1) * WIDTH, :], rows)
                both = both[:WIDTH] * jax.nn.sigmoid(both[WIDTH:])
                send1[a, w, :, :, g * SPAN : (g + 1) * SPAN] = both.reshape(DEPTH, PLANE, SPAN).astype(BF16)

    def along(a, w):
        slot, core = (lax.rem(z, 4) * 2 + c, half) if a == 0 else (z, c)
        for s in (1, 7, 2, 6, 3, 5, 4):
            to = lax.rem(z + s, DEPTH)
            remote(
                send1.at[a, w, to], got1.at[a, w, slot], s1.at[a, w], r1.at[a, w], on_line(to, core)
            ).start()
        if a == 1:
            got1[a, w, slot] = send1[a, w, z]
        else:

            @pl.when(c == half)
            def _():
                got1[a, w, slot] = send1[a, w, z]

            @pl.when(c != half)
            def _():
                remote(
                    send1.at[a, w, z], got1.at[a, w, slot], s1.at[a, w], r1.at[a, w], partner
                ).start()

    def pieces(a, w):
        if a == 1:
            yield send1.at[a, w, pl.ds(0, DEPTH - 1)], None
        else:
            yield send1.at[a, w, pl.ds(0, DEPTH - 1)], c == half
            yield send1.at[a, w], c != half

    def across(a, w):
        with jax.named_scope(f"wait1#{a}{w}"):
            for some, when in pieces(a, w):
                take = remote(some, some, s1.at[a, w], r1.at[a, w], partner)
                if when is None:
                    take.wait_recv()
                else:
                    pl.when(when)(take.wait_recv)
        with jax.named_scope(f"across#{a}{w}"):
            for t in range(6):
                for s in range(DEPTH):
                    mid[t, pl.ds(s, PLANE, stride=DEPTH), :] = got1[
                        a, w, s, :, t * 128 : (t + 1) * 128
                    ].astype(F32)
            for d in range(PLANE):
                for t in range(6):
                    send2[a, w, d, :, t * 128 : (t + 1) * 128] = mid[
                        t, d * DEPTH : (d + 1) * DEPTH, :
                    ].astype(BF16)
            for s in range(1, PLANE):
                to = lax.rem(plane + s, PLANE)
                remote(
                    send2.at[a, w, to], got2.at[a, w, plane], s2.at[a, w], r2.at[a, w], on_plane(to)
                ).start()
            got2[a, w, plane] = send2[a, w, plane]

    def settle(a, w):
        with jax.named_scope(f"wait2#{a}{w}"):
            some = send2.at[a, w, pl.ds(0, PLANE - 1)]
            remote(some, some, s2.at[a, w], r2.at[a, w], partner).wait_recv()
        with jax.named_scope(f"settle#{a}{w}"):
            base, step = (w * PIECE, WAVES * PIECE) if a == 0 else (0, PIECE)
            for yy in range(2):
                for g in range(2):
                    for h in range(2):
                        parts = [
                            got2[a, w, (4 * h + q) * 2 + yy, :, g * SPAN : (g + 1) * SPAN].astype(F32)
                            for q in range(4)
                        ]
                        for b, row in enumerate(regroup(parts)):
                            at = pl.ds(base + yy * WI + 4 * g + b, DEPTH, stride=step)
                            for u in range(3):
                                lines[a, 3 * h + u, at, :] = row[:, u * 128 : (u + 1) * 128]
            for t in range(6):
                cols = slice(t * 128, (t + 1) * 128)
                if a == 0:
                    for s in range(DEPTH):
                        rows = slice(s * step + base, s * step + base + PIECE)
                        left[rows, cols] = lines[0, t, rows, :].astype(BF16)
                else:
                    right[w, pl.ds(pl.multiple_of(c * SIDE, SIDE), SIDE), cols] = lines[
                        1, t, :SIDE, :
                    ].astype(BF16)

    orient(0)
    for w in range(WAVES):
        normalize(w)
        project(0, w)
        if w == 0:
            with jax.named_scope("barrier"):
                pl.semaphore_wait(barrier, 30)
        along(0, w)
    orient(1)
    for w in range(WAVES):
        project(1, w)
        along(1, w)

    with jax.named_scope("gate"):
        fetch_w[4].wait()
        fetch_w[5].wait()
        fetch_g[1].wait()
        gain_col[...] = jnp.broadcast_to(mid_gain[...], (WIDTH, WIDTH)).T

        @pl.loop(0, ROWS // SPAN)
        def _(g):
            rows = pl.ds(pl.multiple_of(g * SPAN, SPAN), SPAN)
            gate[rows, :] = jax.nn.sigmoid(
                jnp.dot(ready[rows, :], weights[5], preferred_element_type=F32)
            )

    right_at = pl.ds(pl.multiple_of(c * SIDE + z * PIECE, PIECE), PIECE)

    def share(w):
        mine = right.at[w, pl.ds(pl.multiple_of(c * SIDE, SIDE), SIDE), :]
        return remote(mine, mine, sf.at[w], rf.at[w], partner)

    def multiply(w):
        with jax.named_scope(f"waitshare#{w}"):
            share(w).wait_recv()
        with jax.named_scope(f"mm#{w}"):
            sums[w] = (nt(right[w], left[...]) * RES ** (-0.5)).astype(BF16)
            for s in range(1, 16):
                t = lax.rem(z * 2 + c + s, 16)
                to_z, to_c = t // 2, lax.rem(t, 2)
                at = pl.ds(pl.multiple_of(to_c * SIDE + to_z * PIECE, PIECE), PIECE)
                remote(
                    sums.at[w, at, :],
                    got3.at[w, z, :, pl.ds(pl.multiple_of(c * HALF, HALF), HALF)],
                    s3.at[w], r3.at[w], on_line(to_z, to_c),
                ).start()
            mine = sums[w, right_at, :]

            @pl.when(c == 0)
            def _():
                got3[w, z, :, :HALF] = mine

            @pl.when(c == 1)
            def _():
                got3[w, z, :, HALF:] = mine

    across(0, 0)
    across(0, 1)
    settle(0, 0)
    across(0, 2)
    settle(0, 1)
    across(1, 0)
    settle(0, 2)
    across(1, 1)
    for w in range(WAVES):
        settle(1, w)
        share(w).start()
        multiply(w)
        if w == 0:
            across(1, 2)

    def gather(w):
        with jax.named_scope(f"wait3#{w}"):
            some = sums.at[w, pl.ds(0, 15 * PIECE), :]
            remote(some, some, s3.at[w], r3.at[w], partner).wait_recv()
        with jax.named_scope(f"gather#{w}"):
            for d in range(DEPTH):
                for t in range(6):
                    mid[t, d * PIECE : (d + 1) * PIECE, :] = got3[
                        w, d, :, t * 128 : (t + 1) * 128
                    ].astype(F32)
            for yy in range(2):
                for g in range(2):
                    for h in range(2):
                        parts = [
                            jnp.concatenate(
                                [
                                    mid[3 * h + u, pl.ds(yy * WI + 4 * g + b, DEPTH, stride=PIECE), :]
                                    for u in range(3)
                                ],
                                axis=1,
                            )
                            for b in range(4)
                        ]
                        for q, row in enumerate(regroup(parts)):
                            send4[w, (4 * h + q) * 2 + yy, :, g * SPAN : (g + 1) * SPAN] = row.astype(BF16)
            for s in range(1, PLANE):
                to = lax.rem(plane + s, PLANE)
                remote(send4.at[w, to], got4.at[w, plane], s4.at[w], r4.at[w], on_plane(to)).start()
            got4[w, plane] = send4[w, plane]

    def finish(w):
        with jax.named_scope(f"wait4#{w}"):
            rest = got4.at[w, pl.ds(0, PLANE - 1)]
            remote(rest, rest, s4.at[w], r4.at[w], partner).wait_recv()
        with jax.named_scope(f"finish#{w}"):
            gains = jnp.concatenate([gain_col[...]] * 3, axis=1)
            for g in range(2):
                v = got4[w, :, :, g * SPAN : (g + 1) * SPAN].astype(F32).reshape(WIDTH, SPAN)
                v = v - jnp.mean(v, axis=0, keepdims=True)
                v = v * lax.rsqrt(jnp.mean(v * v, axis=0, keepdims=True) + 1e-05)
                v = (v * gains).astype(BF16)
                out = lax.dot_general(v, weights[4], (((0,), (0,)), ((), ())), preferred_element_type=F32)
                out = out * gate[w * LANES + g * SPAN : w * LANES + (g + 1) * SPAN, :]
                for b in range(4):
                    for p, i in enumerate(STANDS):
                        flat[pl.ds(i * IB + w * WI + 4 * g + b, WI, stride=IB), :] = out[
                            b * KB + p * WI : b * KB + (p + 1) * WI
                        ]

    gather(0)
    gather(1)
    finish(0)
    gather(2)
    finish(1)
    finish(2)

    with jax.named_scope("store"):

        @pl.loop(0, 4)
        def _(b):
            rows = pl.ds(b * (ROWS // 4), ROWS // 4)
            out_ref[rows, :] = flat[rows, :].astype(BF16)

    def sent(ref, sem):
        remote(ref, ref, sem, r4.at[0], partner).wait_send()

    with jax.named_scope("sent"):
        for w in range(WAVES):
            for a in range(2):
                for some, when in pieces(a, w):
                    if when is None:
                        sent(some, s1.at[a, w])
                    else:
                        pl.when(when)(lambda some=some, a=a, w=w: sent(some, s1.at[a, w]))
                sent(send2.at[a, w, pl.ds(0, PLANE - 1)], s2.at[a, w])
            share(w).wait_send()
            sent(sums.at[w, pl.ds(0, 15 * PIECE), :], s3.at[w])
            sent(send4.at[w, pl.ds(0, PLANE - 1)], s4.at[w])


def body(pair_rows, in_gain, left_weight, right_weight, left_gate, right_gate, mid_gain, out_weight, out_gate):
    dma = pltpu.SemaphoreType.DMA
    vmem = pltpu.VMEM
    out = pl.pallas_call(
        kernel,
        out_shape=jax.ShapeDtypeStruct((ROWS, WIDTH), BF16),
        in_specs=[pl.BlockSpec(memory_space=pltpu.MemorySpace.HBM)] * 9,
        out_specs=pl.BlockSpec(memory_space=vmem),
        scratch_shapes=[
            vmem((WAVES, KB, WI, WIDTH), BF16),
            vmem((1, WIDTH), F32),
            vmem((1, WIDTH), F32),
            vmem((6, WIDTH, WIDTH), BF16),
            vmem((4, WIDTH, WIDTH), F32),
            vmem((ROWS, WIDTH), F32),
            vmem((ROWS, WIDTH), BF16),
            vmem((4 * WIDTH, WIDTH), BF16),
            vmem((2, WAVES, DEPTH, PLANE, LANES), BF16),
            vmem((2, WAVES, DEPTH, PLANE, LANES), BF16),
            vmem((6, DEPTH * PLANE, 128), F32),
            vmem((2, 6, HALF, 128), F32),
            vmem((2, WAVES, PLANE, DEPTH, LANES), BF16),
            vmem((2, WAVES, PLANE, DEPTH, LANES), BF16),
            vmem((HALF, RES), BF16),
            vmem((WAVES, 2 * SIDE, RES), BF16),
            vmem((WAVES, 2 * SIDE, HALF), BF16),
            vmem((WAVES, DEPTH, PIECE, RES), BF16),
            vmem((WAVES, PLANE, 8, LANES), BF16),
            vmem((WAVES, PLANE, 8, LANES), BF16),
            vmem((ROWS, WIDTH), F32),
            vmem((WIDTH, WIDTH), F32),
            dma((WAVES,)), dma((2,)), dma((6,)),
            dma((2, WAVES)), dma((2, WAVES)),
            dma((2, WAVES)), dma((2, WAVES)),
            dma((WAVES,)), dma((WAVES,)),
            dma((WAVES,)), dma((WAVES,)),
            dma((WAVES,)), dma((WAVES,)),
        ],
        compiler_params=pltpu.CompilerParams(
            collective_id=0, has_side_effects=True, vmem_limit_bytes=60 * 2**20
        ),
        name="triangle",
    )(
        pair_rows, in_gain.reshape(1, WIDTH), left_weight, right_weight,
        left_gate, right_gate, mid_gain.reshape(1, WIDTH), out_weight, out_gate,
    )
    return out.reshape(KB, IB, WIDTH)


def solution(mesh):
    placed = (P("north", "east", None), P(), P(), P(), P(), P(), P(), P(), P())
    return jax.shard_map(
        body, mesh=mesh, in_specs=placed, out_specs=P("north", "east", None), check_vma=False
    )
```

```python
import jax
import jax.numpy as jnp
from jax import lax
from jax.experimental import pallas as pl
from jax.experimental.pallas import tpu as pltpu
from jax.sharding import PartitionSpec as P

MESH = pl.DeviceIdType.MESH
F32, BF16 = jnp.float32, jnp.bfloat16

RES, WIDTH = 768, 128
NORTH, EAST, PLANE, DEPTH = 8, 32, 16, 8
KB, IB = RES // NORTH, RES // EAST
ROWS = KB * IB
WAVES, WI = 3, 8
LANES = WI * KB
SPAN = 4 * KB
PIECE = 2 * WI
SIDE = DEPTH * PIECE

STANDS = [y * 48 + c * 24 + w * WI for c in range(2) for w in range(WAVES) for y in range(2)]


def turn(values, amount):
    amount = amount % SPAN
    return values if amount == 0 else pltpu.roll(values, amount, axis=1)


def regroup(parts):
    lane = lax.broadcasted_iota(jnp.int32, parts[0].shape, 1)
    out = []
    for b in range(4):
        row = turn(parts[0], -KB * b)
        for a in range(1, 4):
            row = jnp.where(lane >= KB * a, turn(parts[a], KB * (a - b)), row)
        out.append(row)
    return out


def nt(a, b):
    return lax.dot_general(a, b, (((1,), (1,)), ((), ())), preferred_element_type=F32)


def remote(src, dst, ssem, rsem, where):
    return pltpu.make_async_remote_copy(
        src_ref=src, dst_ref=dst, send_sem=ssem, recv_sem=rsem,
        device_id=where, device_id_type=MESH,
    )


def kernel(
    x_hbm, in_gain_hbm, lw_hbm, rw_hbm, lg_hbm, rg_hbm, mid_gain_hbm, ow_hbm, og_hbm, out_hbm,
    x, in_gain, mid_gain, weights, turned, flat, ready, wt, send1, got1, mid, lines, send2, got2,
    left, right, sums, got3, send4, got4, gate, gain_col, done,
    xs, gs, wsem, s1, r1, s2, r2, sf, rf, s3, r3, s4, r4, ps,
):
    n = lax.axis_index("north")
    e = lax.axis_index("east")
    z, y, c = e // 4, lax.rem(e // 2, 2), lax.rem(e, 2)
    plane = n * 2 + y

    def on_plane(p):
        return (p // 2, (z * 2 + lax.rem(p, 2)) * 2 + c)

    def on_line(to_z):
        return (n, (to_z * 2 + y) * 2 + c)

    partner = (n, (z * 2 + y) * 2 + 1 - c)

    fetch_x = [
        pltpu.make_async_copy(x_hbm.at[:, pl.ds(w * WI, WI), :], x.at[w], xs.at[w])
        for w in range(WAVES)
    ]
    fetch_w = [
        pltpu.make_async_copy(ref, weights.at[p], wsem.at[p])
        for p, ref in enumerate((lw_hbm, lg_hbm, rw_hbm, rg_hbm, ow_hbm, og_hbm))
    ]
    fetch_g = [
        pltpu.make_async_copy(in_gain_hbm, in_gain, gs.at[0]),
        pltpu.make_async_copy(mid_gain_hbm, mid_gain, gs.at[1]),
    ]
    for copy in [fetch_x[0], fetch_g[0], *fetch_w[:2], *fetch_x[1:], *fetch_w[2:], fetch_g[1]]:
        copy.start()

    with jax.named_scope("signal"):
        barrier = pltpu.get_barrier_semaphore()
        partners = [on_plane(lax.rem(plane + s, PLANE)) for s in range(1, PLANE)]
        partners += [on_line(lax.rem(z + s, DEPTH)) for s in range(1, DEPTH)] + [partner]
        for where in partners:
            pl.semaphore_signal(barrier, inc=1, device_id=where, device_id_type=MESH)

    def normalize(w):
        with jax.named_scope(f"norm#{w}"):
            fetch_x[w].wait()
            if w == 0:
                fetch_g[0].wait()
            v = x[w].astype(F32).reshape(LANES, WIDTH)
            v = v - jnp.mean(v, axis=-1, keepdims=True)
            v = v * lax.rsqrt(jnp.mean(v * v, axis=-1, keepdims=True) + 1e-05) * in_gain[...]
            flat[w * LANES : (w + 1) * LANES, :] = v
            for i in range(WI):
                line = [flat[pl.ds(w * LANES + k * WI + i, WI, stride=WI), :] for k in STANDS]
                at = (w * WI + i) * KB
                ready[at : at + KB, :] = jnp.concatenate(line, axis=0).astype(BF16)

    def orient(a):
        for p in range(2 * a, 2 * a + 2):
            fetch_w[p].wait()
            turned[p] = weights[p].astype(F32).T
            for to in range(DEPTH):
                at = p * WIDTH + to * PLANE
                wt[at : at + PLANE, :] = turned[p, pl.ds(to, PLANE, stride=DEPTH), :].astype(BF16)

    def project(a, w):
        with jax.named_scope(f"project#{a}{w}"):
            for g in range(2):
                rows = ready[w * LANES + g * SPAN : w * LANES + (g + 1) * SPAN, :]
                both = nt(wt[2 * a * WIDTH : 2 * (a + 1) * WIDTH, :], rows)
                both = both[:WIDTH] * jax.nn.sigmoid(both[WIDTH:])
                send1[a, w, :, :, g * SPAN : (g + 1) * SPAN] = both.reshape(DEPTH, PLANE, SPAN).astype(BF16)

    def along(a, w):
        for s in (1, 7, 2, 6, 3, 5, 4):
            to = lax.rem(z + s, DEPTH)
            remote(
                send1.at[a, w, to], got1.at[a, w, z], s1.at[a, w], r1.at[a, w], on_line(to)
            ).start()
        got1[a, w, z] = send1[a, w, z]

    def across(a, w):
        with jax.named_scope(f"wait1#{a}{w}"):
            some = send1.at[a, w, pl.ds(0, DEPTH - 1)]
            remote(some, some, s1.at[a, w], r1.at[a, w], partner).wait_recv()
        with jax.named_scope(f"across#{a}{w}"):
            for t in range(6):
                for s in range(DEPTH):
                    mid[t, pl.ds(s, PLANE, stride=DEPTH), :] = got1[
                        a, w, s, :, t * 128 : (t + 1) * 128
                    ].astype(F32)
            for d in range(PLANE):
                for t in range(6):
                    send2[a, w, d, :, t * 128 : (t + 1) * 128] = mid[
                        t, d * DEPTH : (d + 1) * DEPTH, :
                    ].astype(BF16)
            for s in range(1, PLANE):
                to = lax.rem(plane + s, PLANE)
                remote(
                    send2.at[a, w, to], got2.at[a, w, plane], s2.at[a, w], r2.at[a, w], on_plane(to)
                ).start()
            got2[a, w, plane] = send2[a, w, plane]

    def share(w):
        mine = left.at[:, c, w]
        return remote(mine, mine, sf.at[w], rf.at[w], partner)

    def settle(a, w):
        with jax.named_scope(f"wait2#{a}{w}"):
            some = send2.at[a, w, pl.ds(0, PLANE - 1)]
            remote(some, some, s2.at[a, w], r2.at[a, w], partner).wait_recv()
        with jax.named_scope(f"settle#{a}{w}"):
            base, step = (w * PIECE, WAVES * PIECE) if a == 0 else (0, PIECE)
            for yy in range(2):
                for g in range(2):
                    for h in range(2):
                        parts = [
                            got2[a, w, (4 * h + q) * 2 + yy, :, g * SPAN : (g + 1) * SPAN].astype(F32)
                            for q in range(4)
                        ]
                        for b, row in enumerate(regroup(parts)):
                            at = pl.ds(base + yy * WI + 4 * g + b, DEPTH, stride=step)
                            for u in range(3):
                                lines[a, 3 * h + u, at, :] = row[:, u * 128 : (u + 1) * 128]
            for t in range(6):
                cols = slice(t * 128, (t + 1) * 128)
                if a == 0:
                    for s in range(DEPTH):
                        rows = slice(s * step + base, s * step + base + PIECE)
                        left[s, c, w, :, cols] = lines[0, t, rows, :].astype(BF16)
                else:
                    right[w, :, cols] = lines[1, t, :SIDE, :].astype(BF16)
            if a == 0:
                share(w).start()

    orient(0)
    for w in range(WAVES):
        normalize(w)
        project(0, w)
        if w == 0:
            with jax.named_scope("barrier"):
                pl.semaphore_wait(barrier, PLANE + DEPTH - 1)
        along(0, w)
    orient(1)
    for w in range(WAVES):
        project(1, w)
        along(1, w)

    with jax.named_scope("gate"):
        fetch_w[4].wait()
        fetch_w[5].wait()
        fetch_g[1].wait()
        gain_col[...] = jnp.broadcast_to(mid_gain[...], (WIDTH, WIDTH)).T

        @pl.loop(0, ROWS // SPAN)
        def _(g):
            rows = pl.ds(pl.multiple_of(g * SPAN, SPAN), SPAN)
            gate[rows, :] = jax.nn.sigmoid(
                jnp.dot(ready[rows, :], weights[5], preferred_element_type=F32)
            )

    def multiply(w):
        if w == 0:
            with jax.named_scope("waitshare"):
                for ww in range(WAVES):
                    share(ww).wait_recv()
        with jax.named_scope(f"mm#{w}"):
            sums[w] = (nt(right[w], left[...].reshape(RES, RES)) * RES ** (-0.5)).astype(BF16)
            for s in (1, 7, 2, 6, 3, 5, 4):
                to = lax.rem(z + s, DEPTH)
                at = pl.ds(pl.multiple_of(to * PIECE, PIECE), PIECE)
                remote(sums.at[w, at, :], got3.at[w, z], s3.at[w], r3.at[w], on_line(to)).start()
            got3[w, z] = sums[w, pl.ds(pl.multiple_of(z * PIECE, PIECE), PIECE), :]

    across(0, 0)
    across(0, 1)
    settle(0, 0)
    across(0, 2)
    settle(0, 1)
    across(1, 0)
    settle(0, 2)
    across(1, 1)
    settle(1, 0)
    multiply(0)
    across(1, 2)
    settle(1, 1)
    multiply(1)
    settle(1, 2)
    multiply(2)

    def gather(w):
        with jax.named_scope(f"wait3#{w}"):
            some = sums.at[w, pl.ds(0, 7 * PIECE), :]
            remote(some, some, s3.at[w], r3.at[w], partner).wait_recv()
        with jax.named_scope(f"gather#{w}"):
            for d in range(DEPTH):
                for t in range(6):
                    mid[t, d * PIECE : (d + 1) * PIECE, :] = got3[
                        w, d, :, t * 128 : (t + 1) * 128
                    ].astype(F32)
            for yy in range(2):
                for g in range(2):
                    for h in range(2):
                        parts = [
                            jnp.concatenate(
                                [
                                    mid[3 * h + u, pl.ds(yy * WI + 4 * g + b, DEPTH, stride=PIECE), :]
                                    for u in range(3)
                                ],
                                axis=1,
                            )
                            for b in range(4)
                        ]
                        for q, row in enumerate(regroup(parts)):
                            send4[w, (4 * h + q) * 2 + yy, :, g * SPAN : (g + 1) * SPAN] = row.astype(BF16)
            for s in range(1, PLANE):
                to = lax.rem(plane + s, PLANE)
                remote(send4.at[w, to], got4.at[w, plane], s4.at[w], r4.at[w], on_plane(to)).start()
            got4[w, plane] = send4[w, plane]

    put = [
        pltpu.make_async_copy(done.at[w], out_hbm.at[:, pl.ds(w * WI, WI), :], ps.at[w])
        for w in range(WAVES)
    ]

    def finish(w):
        with jax.named_scope(f"wait4#{w}"):
            rest = got4.at[w, pl.ds(0, PLANE - 1)]
            remote(rest, rest, s4.at[w], r4.at[w], partner).wait_recv()
        with jax.named_scope(f"finish#{w}"):
            gains = jnp.concatenate([gain_col[...]] * 3, axis=1)
            for g in range(2):
                v = got4[w, :, :, g * SPAN : (g + 1) * SPAN].astype(F32).reshape(WIDTH, SPAN)
                v = v - jnp.mean(v, axis=0, keepdims=True)
                v = v * lax.rsqrt(jnp.mean(v * v, axis=0, keepdims=True) + 1e-05)
                v = (v * gains).astype(BF16)
                out = lax.dot_general(v, weights[4], (((0,), (0,)), ((), ())), preferred_element_type=F32)
                out = out * gate[w * LANES + g * SPAN : w * LANES + (g + 1) * SPAN, :]
                for b in range(4):
                    for p, i in enumerate(STANDS):
                        flat[pl.ds(w * LANES + i * WI + 4 * g + b, WI, stride=WI), :] = out[
                            b * KB + p * WI : b * KB + (p + 1) * WI
                        ]
            done[w] = flat[w * LANES : (w + 1) * LANES, :].reshape(KB, WI, WIDTH).astype(BF16)
            put[w].start()

    gather(0)
    gather(1)
    finish(0)
    gather(2)
    finish(1)
    finish(2)

    def sent(ref, sem):
        remote(ref, ref, sem, r4.at[0], partner).wait_send()

    with jax.named_scope("sent"):
        for w in range(WAVES):
            put[w].wait()
            for a in range(2):
                sent(send1.at[a, w, pl.ds(0, DEPTH - 1)], s1.at[a, w])
                sent(send2.at[a, w, pl.ds(0, PLANE - 1)], s2.at[a, w])
            share(w).wait_send()
            sent(sums.at[w, pl.ds(0, 7 * PIECE), :], s3.at[w])
            sent(send4.at[w, pl.ds(0, PLANE - 1)], s4.at[w])


def body(pair_rows, in_gain, left_weight, right_weight, left_gate, right_gate, mid_gain, out_weight, out_gate):
    dma = pltpu.SemaphoreType.DMA
    vmem = pltpu.VMEM
    return pl.pallas_call(
        kernel,
        out_shape=jax.ShapeDtypeStruct((KB, IB, WIDTH), BF16),
        in_specs=[pl.BlockSpec(memory_space=pltpu.MemorySpace.HBM)] * 9,
        out_specs=pl.BlockSpec(memory_space=pltpu.MemorySpace.HBM),
        scratch_shapes=[
            vmem((WAVES, KB, WI, WIDTH), BF16),
            vmem((1, WIDTH), F32),
            vmem((1, WIDTH), F32),
            vmem((6, WIDTH, WIDTH), BF16),
            vmem((4, WIDTH, WIDTH), F32),
            vmem((ROWS, WIDTH), F32),
            vmem((ROWS, WIDTH), BF16),
            vmem((4 * WIDTH, WIDTH), BF16),
            vmem((2, WAVES, DEPTH, PLANE, LANES), BF16),
            vmem((2, WAVES, DEPTH, PLANE, LANES), BF16),
            vmem((6, DEPTH * PLANE, 128), F32),
            vmem((2, 6, RES // 2, 128), F32),
            vmem((2, WAVES, PLANE, DEPTH, LANES), BF16),
            vmem((2, WAVES, PLANE, DEPTH, LANES), BF16),
            vmem((DEPTH, 2, WAVES, PIECE, RES), BF16),
            vmem((WAVES, SIDE, RES), BF16),
            vmem((WAVES, SIDE, RES), BF16),
            vmem((WAVES, DEPTH, PIECE, RES), BF16),
            vmem((WAVES, PLANE, 8, LANES), BF16),
            vmem((WAVES, PLANE, 8, LANES), BF16),
            vmem((ROWS, WIDTH), F32),
            vmem((WIDTH, WIDTH), F32),
            vmem((WAVES, KB, WI, WIDTH), BF16),
            dma((WAVES,)), dma((2,)), dma((6,)),
            dma((2, WAVES)), dma((2, WAVES)),
            dma((2, WAVES)), dma((2, WAVES)),
            dma((WAVES,)), dma((WAVES,)),
            dma((WAVES,)), dma((WAVES,)),
            dma((WAVES,)), dma((WAVES,)),
            dma((WAVES,)),
        ],
        compiler_params=pltpu.CompilerParams(
            collective_id=0, has_side_effects=True, vmem_limit_bytes=60 * 2**20
        ),
        name="triangle",
    )(
        pair_rows, in_gain.reshape(1, WIDTH), left_weight, right_weight,
        left_gate, right_gate, mid_gain.reshape(1, WIDTH), out_weight, out_gate,
    )


def solution(mesh):
    placed = (P("north", "east", None), P(), P(), P(), P(), P(), P(), P(), P())
    return jax.shard_map(
        body, mesh=mesh, in_specs=placed, out_specs=P("north", "east", None), check_vma=False
    )
```

```python
import jax
import jax.numpy as jnp
from jax import lax
from jax.experimental import pallas as pl
from jax.experimental.pallas import tpu as pltpu
from jax.sharding import PartitionSpec as P

MESH = pl.DeviceIdType.MESH
F32, BF16 = jnp.float32, jnp.bfloat16

RES, WIDTH = 768, 128
NORTH, EAST, PLANE, DEPTH = 8, 32, 16, 8
KB, IB = RES // NORTH, RES // EAST
ROWS = KB * IB
WAVES, WI = 3, 8
LANES = WI * KB
SPAN = 4 * KB
PIECE = 2 * WI
SIDE = DEPTH * PIECE

STANDS = [y * 48 + c * 24 + w * WI for c in range(2) for w in range(WAVES) for y in range(2)]


ACROSS = sorted(
    ((dx, dy) for dx in range(4) for dy in range(4) if dx or dy),
    key=lambda step: -sum(min(d, 4 - d) for d in step),
)
ALONG = (4, 3, 5, 2, 6, 1, 7)


def turn(values, amount):
    amount = amount % SPAN
    return values if amount == 0 else pltpu.roll(values, amount, axis=1)


def regroup(parts):
    lane = lax.broadcasted_iota(jnp.int32, parts[0].shape, 1)
    out = []
    for b in range(4):
        row = turn(parts[0], -KB * b)
        for a in range(1, 4):
            row = jnp.where(lane >= KB * a, turn(parts[a], KB * (a - b)), row)
        out.append(row)
    return out


def nt(a, b):
    return lax.dot_general(a, b, (((1,), (1,)), ((), ())), preferred_element_type=F32)


def remote(src, dst, ssem, rsem, where):
    return pltpu.make_async_remote_copy(
        src_ref=src, dst_ref=dst, send_sem=ssem, recv_sem=rsem,
        device_id=where, device_id_type=MESH,
    )


def kernel(
    x_hbm, in_gain_hbm, lw_hbm, rw_hbm, lg_hbm, rg_hbm, mid_gain_hbm, ow_hbm, og_hbm, out_hbm,
    x, in_gain, mid_gain, weights, turned, flat, ready, wt, send1, got1, mid, lines, send2, got2,
    left, right, sums, got3, send4, got4, gate, gain_col, done,
    xs, gs, wsem, s1, r1, s2, r2, sf, rf, s3, r3, s4, r4, ps,
):
    n = lax.axis_index("north")
    e = lax.axis_index("east")
    z, y, c = e // 4, lax.rem(e // 2, 2), lax.rem(e, 2)
    plane = n * 2 + y

    px, py = lax.rem(n, 4), (n // 4) * 2 + y

    def on_plane(step):
        x_to, y_to = lax.rem(px + step[0], 4), lax.rem(py + step[1], 4)
        n_to, y_to = (y_to // 2) * 4 + x_to, lax.rem(y_to, 2)
        return n_to * 2 + y_to, (n_to, (z * 2 + y_to) * 2 + c)

    def on_line(to_z):
        return (n, (to_z * 2 + y) * 2 + c)

    partner = (n, (z * 2 + y) * 2 + 1 - c)

    fetch_x = [
        pltpu.make_async_copy(x_hbm.at[:, pl.ds(w * WI, WI), :], x.at[w], xs.at[w])
        for w in range(WAVES)
    ]
    fetch_w = [
        pltpu.make_async_copy(ref, weights.at[p], wsem.at[p])
        for p, ref in enumerate((lw_hbm, lg_hbm, rw_hbm, rg_hbm, ow_hbm, og_hbm))
    ]
    fetch_g = [
        pltpu.make_async_copy(in_gain_hbm, in_gain, gs.at[0]),
        pltpu.make_async_copy(mid_gain_hbm, mid_gain, gs.at[1]),
    ]
    for copy in [fetch_x[0], fetch_g[0], *fetch_w[:2], *fetch_x[1:], *fetch_w[2:], fetch_g[1]]:
        copy.start()

    with jax.named_scope("signal"):
        barrier = pltpu.get_barrier_semaphore()
        partners = [on_plane(step)[1] for step in ACROSS]
        partners += [on_line(lax.rem(z + s, DEPTH)) for s in range(1, DEPTH)] + [partner]
        for where in partners:
            pl.semaphore_signal(barrier, inc=1, device_id=where, device_id_type=MESH)

    def normalize(w):
        with jax.named_scope(f"norm#{w}"):
            fetch_x[w].wait()
            if w == 0:
                fetch_g[0].wait()
            v = x[w].astype(F32).reshape(LANES, WIDTH)
            v = v - jnp.mean(v, axis=-1, keepdims=True)
            v = v * lax.rsqrt(jnp.mean(v * v, axis=-1, keepdims=True) + 1e-05) * in_gain[...]
            flat[w * LANES : (w + 1) * LANES, :] = v
            for i in range(WI):
                line = [flat[pl.ds(w * LANES + k * WI + i, WI, stride=WI), :] for k in STANDS]
                at = (w * WI + i) * KB
                ready[at : at + KB, :] = jnp.concatenate(line, axis=0).astype(BF16)

    def orient(a):
        for p in range(2 * a, 2 * a + 2):
            fetch_w[p].wait()
            turned[p] = weights[p].astype(F32).T
            for to in range(DEPTH):
                at = p * WIDTH + to * PLANE
                wt[at : at + PLANE, :] = turned[p, pl.ds(to, PLANE, stride=DEPTH), :].astype(BF16)

    def project(a, w):
        with jax.named_scope(f"project#{a}{w}"):
            for g in range(2):
                rows = ready[w * LANES + g * SPAN : w * LANES + (g + 1) * SPAN, :]
                both = nt(wt[2 * a * WIDTH : 2 * (a + 1) * WIDTH, :], rows)
                both = both[:WIDTH] * jax.nn.sigmoid(both[WIDTH:])
                send1[a, w, :, :, g * SPAN : (g + 1) * SPAN] = both.reshape(DEPTH, PLANE, SPAN).astype(BF16)

    def along(a, w):
        for s in ALONG:
            to = lax.rem(z + s, DEPTH)
            remote(
                send1.at[a, w, to], got1.at[a, w, z], s1.at[a, w], r1.at[a, w], on_line(to)
            ).start()
        got1[a, w, z] = send1[a, w, z]

    def across(a, w):
        with jax.named_scope(f"wait1#{a}{w}"):
            some = send1.at[a, w, pl.ds(0, DEPTH - 1)]
            remote(some, some, s1.at[a, w], r1.at[a, w], partner).wait_recv()
        with jax.named_scope(f"across#{a}{w}"):
            for t in range(6):
                for s in range(DEPTH):
                    mid[t, pl.ds(s, PLANE, stride=DEPTH), :] = got1[
                        a, w, s, :, t * 128 : (t + 1) * 128
                    ].astype(F32)
            for d in range(PLANE):
                for t in range(6):
                    send2[a, w, d, :, t * 128 : (t + 1) * 128] = mid[
                        t, d * DEPTH : (d + 1) * DEPTH, :
                    ].astype(BF16)
            for step in ACROSS:
                to, where = on_plane(step)
                remote(
                    send2.at[a, w, to], got2.at[a, w, plane], s2.at[a, w], r2.at[a, w], where
                ).start()
            got2[a, w, plane] = send2[a, w, plane]

    def share(w):
        mine = left.at[:, c, w]
        return remote(mine, mine, sf.at[w], rf.at[w], partner)

    def settle(a, w):
        with jax.named_scope(f"wait2#{a}{w}"):
            some = send2.at[a, w, pl.ds(0, PLANE - 1)]
            remote(some, some, s2.at[a, w], r2.at[a, w], partner).wait_recv()
        with jax.named_scope(f"settle#{a}{w}"):
            base, step = (w * PIECE, WAVES * PIECE) if a == 0 else (0, PIECE)
            for yy in range(2):
                for g in range(2):
                    for h in range(2):
                        parts = [
                            got2[a, w, (4 * h + q) * 2 + yy, :, g * SPAN : (g + 1) * SPAN].astype(F32)
                            for q in range(4)
                        ]
                        for b, row in enumerate(regroup(parts)):
                            at = pl.ds(base + yy * WI + 4 * g + b, DEPTH, stride=step)
                            for u in range(3):
                                lines[a, 3 * h + u, at, :] = row[:, u * 128 : (u + 1) * 128]
            for t in range(6):
                cols = slice(t * 128, (t + 1) * 128)
                if a == 0:
                    for s in range(DEPTH):
                        rows = slice(s * step + base, s * step + base + PIECE)
                        left[s, c, w, :, cols] = lines[0, t, rows, :].astype(BF16)
                else:
                    right[w, :, cols] = lines[1, t, :SIDE, :].astype(BF16)
            if a == 0:
                share(w).start()

    orient(0)
    for w in range(WAVES):
        normalize(w)
        project(0, w)
        if w == 0:
            with jax.named_scope("barrier"):
                pl.semaphore_wait(barrier, PLANE + DEPTH - 1)
        along(0, w)
    orient(1)
    for w in range(WAVES):
        project(1, w)
        along(1, w)

    with jax.named_scope("gate"):
        fetch_w[4].wait()
        fetch_w[5].wait()
        fetch_g[1].wait()
        gain_col[...] = jnp.broadcast_to(mid_gain[...], (WIDTH, WIDTH)).T

        @pl.loop(0, ROWS // SPAN)
        def _(g):
            rows = pl.ds(pl.multiple_of(g * SPAN, SPAN), SPAN)
            gate[rows, :] = jax.nn.sigmoid(
                jnp.dot(ready[rows, :], weights[5], preferred_element_type=F32)
            )

    def multiply(w):
        if w == 0:
            with jax.named_scope("waitshare"):
                for ww in range(WAVES):
                    share(ww).wait_recv()
        with jax.named_scope(f"mm#{w}"):
            sums[w] = (nt(right[w], left[...].reshape(RES, RES)) * RES ** (-0.5)).astype(BF16)
            for s in ALONG:
                to = lax.rem(z + s, DEPTH)
                at = pl.ds(pl.multiple_of(to * PIECE, PIECE), PIECE)
                remote(sums.at[w, at, :], got3.at[w, z], s3.at[w], r3.at[w], on_line(to)).start()
            got3[w, z] = sums[w, pl.ds(pl.multiple_of(z * PIECE, PIECE), PIECE), :]

    across(0, 0)
    across(0, 1)
    settle(0, 0)
    across(0, 2)
    settle(0, 1)
    across(1, 0)
    settle(0, 2)
    across(1, 1)
    settle(1, 0)
    multiply(0)
    across(1, 2)
    settle(1, 1)
    multiply(1)
    settle(1, 2)
    multiply(2)

    def gather(w):
        with jax.named_scope(f"wait3#{w}"):
            some = sums.at[w, pl.ds(0, 7 * PIECE), :]
            remote(some, some, s3.at[w], r3.at[w], partner).wait_recv()
        with jax.named_scope(f"gather#{w}"):
            for d in range(DEPTH):
                for t in range(6):
                    mid[t, d * PIECE : (d + 1) * PIECE, :] = got3[
                        w, d, :, t * 128 : (t + 1) * 128
                    ].astype(F32)
            for yy in range(2):
                for g in range(2):
                    for h in range(2):
                        parts = [
                            jnp.concatenate(
                                [
                                    mid[3 * h + u, pl.ds(yy * WI + 4 * g + b, DEPTH, stride=PIECE), :]
                                    for u in range(3)
                                ],
                                axis=1,
                            )
                            for b in range(4)
                        ]
                        for q, row in enumerate(regroup(parts)):
                            send4[w, (4 * h + q) * 2 + yy, :, g * SPAN : (g + 1) * SPAN] = row.astype(BF16)
            for step in ACROSS:
                to, where = on_plane(step)
                remote(send4.at[w, to], got4.at[w, plane], s4.at[w], r4.at[w], where).start()
            got4[w, plane] = send4[w, plane]

    put = [
        pltpu.make_async_copy(done.at[w], out_hbm.at[:, pl.ds(w * WI, WI), :], ps.at[w])
        for w in range(WAVES)
    ]

    def finish(w):
        with jax.named_scope(f"wait4#{w}"):
            rest = got4.at[w, pl.ds(0, PLANE - 1)]
            remote(rest, rest, s4.at[w], r4.at[w], partner).wait_recv()
        with jax.named_scope(f"finish#{w}"):
            gains = jnp.concatenate([gain_col[...]] * 3, axis=1)
            for g in range(2):
                v = got4[w, :, :, g * SPAN : (g + 1) * SPAN].astype(F32).reshape(WIDTH, SPAN)
                v = v - jnp.mean(v, axis=0, keepdims=True)
                v = v * lax.rsqrt(jnp.mean(v * v, axis=0, keepdims=True) + 1e-05)
                v = (v * gains).astype(BF16)
                out = lax.dot_general(v, weights[4], (((0,), (0,)), ((), ())), preferred_element_type=F32)
                out = out * gate[w * LANES + g * SPAN : w * LANES + (g + 1) * SPAN, :]
                for b in range(4):
                    for p, i in enumerate(STANDS):
                        flat[pl.ds(w * LANES + i * WI + 4 * g + b, WI, stride=WI), :] = out[
                            b * KB + p * WI : b * KB + (p + 1) * WI
                        ]
            done[w] = flat[w * LANES : (w + 1) * LANES, :].reshape(KB, WI, WIDTH).astype(BF16)
            put[w].start()

    gather(0)
    gather(1)
    finish(0)
    gather(2)
    finish(1)
    finish(2)

    def sent(ref, sem):
        remote(ref, ref, sem, r4.at[0], partner).wait_send()

    with jax.named_scope("sent"):
        for w in range(WAVES):
            put[w].wait()
            for a in range(2):
                sent(send1.at[a, w, pl.ds(0, DEPTH - 1)], s1.at[a, w])
                sent(send2.at[a, w, pl.ds(0, PLANE - 1)], s2.at[a, w])
            share(w).wait_send()
            sent(sums.at[w, pl.ds(0, 7 * PIECE), :], s3.at[w])
            sent(send4.at[w, pl.ds(0, PLANE - 1)], s4.at[w])


def body(pair_rows, in_gain, left_weight, right_weight, left_gate, right_gate, mid_gain, out_weight, out_gate):
    dma = pltpu.SemaphoreType.DMA
    vmem = pltpu.VMEM
    return pl.pallas_call(
        kernel,
        out_shape=jax.ShapeDtypeStruct((KB, IB, WIDTH), BF16),
        in_specs=[pl.BlockSpec(memory_space=pltpu.MemorySpace.HBM)] * 9,
        out_specs=pl.BlockSpec(memory_space=pltpu.MemorySpace.HBM),
        scratch_shapes=[
            vmem((WAVES, KB, WI, WIDTH), BF16),
            vmem((1, WIDTH), F32),
            vmem((1, WIDTH), F32),
            vmem((6, WIDTH, WIDTH), BF16),
            vmem((4, WIDTH, WIDTH), F32),
            vmem((ROWS, WIDTH), F32),
            vmem((ROWS, WIDTH), BF16),
            vmem((4 * WIDTH, WIDTH), BF16),
            vmem((2, WAVES, DEPTH, PLANE, LANES), BF16),
            vmem((2, WAVES, DEPTH, PLANE, LANES), BF16),
            vmem((6, DEPTH * PLANE, 128), F32),
            vmem((2, 6, RES // 2, 128), F32),
            vmem((2, WAVES, PLANE, DEPTH, LANES), BF16),
            vmem((2, WAVES, PLANE, DEPTH, LANES), BF16),
            vmem((DEPTH, 2, WAVES, PIECE, RES), BF16),
            vmem((WAVES, SIDE, RES), BF16),
            vmem((WAVES, SIDE, RES), BF16),
            vmem((WAVES, DEPTH, PIECE, RES), BF16),
            vmem((WAVES, PLANE, 8, LANES), BF16),
            vmem((WAVES, PLANE, 8, LANES), BF16),
            vmem((ROWS, WIDTH), F32),
            vmem((WIDTH, WIDTH), F32),
            vmem((WAVES, KB, WI, WIDTH), BF16),
            dma((WAVES,)), dma((2,)), dma((6,)),
            dma((2, WAVES)), dma((2, WAVES)),
            dma((2, WAVES)), dma((2, WAVES)),
            dma((WAVES,)), dma((WAVES,)),
            dma((WAVES,)), dma((WAVES,)),
            dma((WAVES,)), dma((WAVES,)),
            dma((WAVES,)),
        ],
        compiler_params=pltpu.CompilerParams(
            collective_id=0, has_side_effects=True, vmem_limit_bytes=60 * 2**20
        ),
        name="triangle",
    )(
        pair_rows, in_gain.reshape(1, WIDTH), left_weight, right_weight,
        left_gate, right_gate, mid_gain.reshape(1, WIDTH), out_weight, out_gate,
    )


def solution(mesh):
    placed = (P("north", "east", None), P(), P(), P(), P(), P(), P(), P(), P())
    return jax.shard_map(
        body, mesh=mesh, in_specs=placed, out_specs=P("north", "east", None), check_vma=False
    )
```

```python
import jax
import jax.numpy as jnp
from jax import lax
from jax.experimental import pallas as pl
from jax.experimental.pallas import tpu as pltpu
from jax.sharding import PartitionSpec as P

MESH = pl.DeviceIdType.MESH
F32, BF16 = jnp.float32, jnp.bfloat16

RES, WIDTH = 768, 128
NORTH, EAST, PLANE, DEPTH = 8, 32, 16, 8
KB, IB = RES // NORTH, RES // EAST
ROWS = KB * IB
WAVES, WI = 3, 8
LANES = WI * KB
SPAN = 4 * KB
PIECE = 2 * WI
SIDE = DEPTH * PIECE

STANDS = [y * 48 + c * 24 + w * WI for c in range(2) for w in range(WAVES) for y in range(2)]


ACROSS = sorted(
    ((dx, dy) for dx in range(4) for dy in range(4) if dx or dy),
    key=lambda step: -sum(min(d, 4 - d) for d in step),
)
ALONG = (4, 3, 5, 2, 6, 1, 7)


def turn(values, amount):
    amount = amount % SPAN
    return values if amount == 0 else pltpu.roll(values, amount, axis=1)


def regroup(parts):
    lane = lax.broadcasted_iota(jnp.int32, parts[0].shape, 1)
    out = []
    for b in range(4):
        row = turn(parts[0], -KB * b)
        for a in range(1, 4):
            row = jnp.where(lane >= KB * a, turn(parts[a], KB * (a - b)), row)
        out.append(row)
    return out


def nt(a, b):
    return lax.dot_general(a, b, (((1,), (1,)), ((), ())), preferred_element_type=F32)


def remote(src, dst, ssem, rsem, where):
    return pltpu.make_async_remote_copy(
        src_ref=src, dst_ref=dst, send_sem=ssem, recv_sem=rsem,
        device_id=where, device_id_type=MESH,
    )


def kernel(
    x_hbm, in_gain_hbm, lw_hbm, rw_hbm, lg_hbm, rg_hbm, mid_gain_hbm, ow_hbm, og_hbm, out_hbm,
    x, in_gain, mid_gain, weights, turned, flat, ready, wt, send1, got1, mid, lines, send2, got2,
    left, right, sums, got3, send4, got4, gate, gain_col,
    xs, gs, wsem, s1, r1, s2, r2, sf, rf, s3, r3, s4, r4,
):
    n = lax.axis_index("north")
    e = lax.axis_index("east")
    z, y, c = e // 4, lax.rem(e // 2, 2), lax.rem(e, 2)
    plane = n * 2 + y

    px, py = lax.rem(n, 4), (n // 4) * 2 + y

    def on_plane(step):
        x_to, y_to = lax.rem(px + step[0], 4), lax.rem(py + step[1], 4)
        n_to, y_to = (y_to // 2) * 4 + x_to, lax.rem(y_to, 2)
        return n_to * 2 + y_to, (n_to, (z * 2 + y_to) * 2 + c)

    def on_line(to_z):
        return (n, (to_z * 2 + y) * 2 + c)

    partner = (n, (z * 2 + y) * 2 + 1 - c)

    fetch_x = [
        pltpu.make_async_copy(x_hbm.at[:, pl.ds(w * WI, WI), :], x.at[w], xs.at[w])
        for w in range(WAVES)
    ]
    fetch_w = [
        pltpu.make_async_copy(ref, weights.at[p], wsem.at[p])
        for p, ref in enumerate((lw_hbm, lg_hbm, rw_hbm, rg_hbm, ow_hbm, og_hbm))
    ]
    fetch_g = [
        pltpu.make_async_copy(in_gain_hbm, in_gain, gs.at[0]),
        pltpu.make_async_copy(mid_gain_hbm, mid_gain, gs.at[1]),
    ]
    for copy in [fetch_x[0], fetch_g[0], *fetch_w[:2], *fetch_x[1:], *fetch_w[2:], fetch_g[1]]:
        copy.start()

    with jax.named_scope("signal"):
        barrier = pltpu.get_barrier_semaphore()
        partners = [on_plane(step)[1] for step in ACROSS]
        partners += [on_line(lax.rem(z + s, DEPTH)) for s in range(1, DEPTH)] + [partner]
        for where in partners:
            pl.semaphore_signal(barrier, inc=1, device_id=where, device_id_type=MESH)

    def normalize(w):
        with jax.named_scope(f"norm#{w}"):
            fetch_x[w].wait()
            if w == 0:
                fetch_g[0].wait()
            v = x[w].astype(F32).reshape(LANES, WIDTH)
            v = v - jnp.mean(v, axis=-1, keepdims=True)
            v = v * lax.rsqrt(jnp.mean(v * v, axis=-1, keepdims=True) + 1e-05) * in_gain[...]
            flat[w * LANES : (w + 1) * LANES, :] = v
            for i in range(WI):
                line = [flat[pl.ds(w * LANES + k * WI + i, WI, stride=WI), :] for k in STANDS]
                at = (w * WI + i) * KB
                ready[at : at + KB, :] = jnp.concatenate(line, axis=0).astype(BF16)

    def orient(a):
        for p in range(2 * a, 2 * a + 2):
            fetch_w[p].wait()
            turned[p] = weights[p].astype(F32).T
            for to in range(DEPTH):
                at = p * WIDTH + to * PLANE
                wt[at : at + PLANE, :] = turned[p, pl.ds(to, PLANE, stride=DEPTH), :].astype(BF16)

    def project(a, w):
        with jax.named_scope(f"project#{a}{w}"):
            for g in range(2):
                rows = ready[w * LANES + g * SPAN : w * LANES + (g + 1) * SPAN, :]
                both = nt(wt[2 * a * WIDTH : 2 * (a + 1) * WIDTH, :], rows)
                both = both[:WIDTH] * jax.nn.sigmoid(both[WIDTH:])
                send1[a, w, :, :, g * SPAN : (g + 1) * SPAN] = both.reshape(DEPTH, PLANE, SPAN).astype(BF16)

    def along(a, w):
        for s in ALONG:
            to = lax.rem(z + s, DEPTH)
            remote(
                send1.at[a, w, to], got1.at[a, w, z], s1.at[a, w], r1.at[a, w], on_line(to)
            ).start()
        got1[a, w, z] = send1[a, w, z]

    def across(a, w):
        with jax.named_scope(f"wait1#{a}{w}"):
            some = send1.at[a, w, pl.ds(0, DEPTH - 1)]
            remote(some, some, s1.at[a, w], r1.at[a, w], partner).wait_recv()
        with jax.named_scope(f"across#{a}{w}"):
            for t in range(6):
                for s in range(DEPTH):
                    mid[t, pl.ds(s, PLANE, stride=DEPTH), :] = got1[
                        a, w, s, :, t * 128 : (t + 1) * 128
                    ].astype(F32)
            for d in range(PLANE):
                for t in range(6):
                    send2[a, w, d, :, t * 128 : (t + 1) * 128] = mid[
                        t, d * DEPTH : (d + 1) * DEPTH, :
                    ].astype(BF16)
            for step in ACROSS:
                to, where = on_plane(step)
                remote(
                    send2.at[a, w, to], got2.at[a, w, plane], s2.at[a, w], r2.at[a, w], where
                ).start()
            got2[a, w, plane] = send2[a, w, plane]

    def share(w):
        mine = left.at[:, c, w]
        return remote(mine, mine, sf.at[w], rf.at[w], partner)

    def settle(a, w):
        with jax.named_scope(f"wait2#{a}{w}"):
            some = send2.at[a, w, pl.ds(0, PLANE - 1)]
            remote(some, some, s2.at[a, w], r2.at[a, w], partner).wait_recv()
        with jax.named_scope(f"settle#{a}{w}"):
            base, step = (w * PIECE, WAVES * PIECE) if a == 0 else (0, PIECE)
            for yy in range(2):
                for g in range(2):
                    for h in range(2):
                        parts = [
                            got2[a, w, (4 * h + q) * 2 + yy, :, g * SPAN : (g + 1) * SPAN].astype(F32)
                            for q in range(4)
                        ]
                        for b, row in enumerate(regroup(parts)):
                            at = pl.ds(base + yy * WI + 4 * g + b, DEPTH, stride=step)
                            for u in range(3):
                                lines[a, 3 * h + u, at, :] = row[:, u * 128 : (u + 1) * 128]
            for t in range(6):
                cols = slice(t * 128, (t + 1) * 128)
                if a == 0:
                    for s in range(DEPTH):
                        rows = slice(s * step + base, s * step + base + PIECE)
                        left[s, c, w, :, cols] = lines[0, t, rows, :].astype(BF16)
                else:
                    right[w, :, cols] = lines[1, t, :SIDE, :].astype(BF16)
            if a == 0:
                share(w).start()

    orient(0)
    for w in range(WAVES):
        normalize(w)
        project(0, w)
        if w == 0:
            with jax.named_scope("barrier"):
                pl.semaphore_wait(barrier, PLANE + DEPTH - 1)
        along(0, w)
    orient(1)
    for w in range(WAVES):
        project(1, w)
        along(1, w)

    with jax.named_scope("gate"):
        fetch_w[4].wait()
        fetch_w[5].wait()
        fetch_g[1].wait()
        gain_col[...] = jnp.broadcast_to(mid_gain[...], (WIDTH, WIDTH)).T

        @pl.loop(0, ROWS // SPAN)
        def _(g):
            rows = pl.ds(pl.multiple_of(g * SPAN, SPAN), SPAN)
            gate[rows, :] = jax.nn.sigmoid(
                jnp.dot(ready[rows, :], weights[5], preferred_element_type=F32)
            )

    def multiply(w):
        if w == 0:
            with jax.named_scope("waitshare"):
                for ww in range(WAVES):
                    share(ww).wait_recv()
        with jax.named_scope(f"mm#{w}"):
            sums[w] = (nt(right[w], left[...].reshape(RES, RES)) * RES ** (-0.5)).astype(BF16)
            for s in ALONG:
                to = lax.rem(z + s, DEPTH)
                at = pl.ds(pl.multiple_of(to * PIECE, PIECE), PIECE)
                remote(sums.at[w, at, :], got3.at[w, z], s3.at[w], r3.at[w], on_line(to)).start()
            got3[w, z] = sums[w, pl.ds(pl.multiple_of(z * PIECE, PIECE), PIECE), :]

    across(0, 0)
    across(0, 1)
    settle(0, 0)
    across(0, 2)
    settle(0, 1)
    across(1, 0)
    settle(0, 2)
    across(1, 1)
    settle(1, 0)
    multiply(0)
    across(1, 2)
    settle(1, 1)
    multiply(1)
    settle(1, 2)
    multiply(2)

    def gather(w):
        with jax.named_scope(f"wait3#{w}"):
            some = sums.at[w, pl.ds(0, 7 * PIECE), :]
            remote(some, some, s3.at[w], r3.at[w], partner).wait_recv()
        with jax.named_scope(f"gather#{w}"):
            for d in range(DEPTH):
                for t in range(6):
                    mid[t, d * PIECE : (d + 1) * PIECE, :] = got3[
                        w, d, :, t * 128 : (t + 1) * 128
                    ].astype(F32)
            for yy in range(2):
                for g in range(2):
                    for h in range(2):
                        parts = [
                            jnp.concatenate(
                                [
                                    mid[3 * h + u, pl.ds(yy * WI + 4 * g + b, DEPTH, stride=PIECE), :]
                                    for u in range(3)
                                ],
                                axis=1,
                            )
                            for b in range(4)
                        ]
                        for q, row in enumerate(regroup(parts)):
                            send4[w, (4 * h + q) * 2 + yy, :, g * SPAN : (g + 1) * SPAN] = row.astype(BF16)
            for step in ACROSS:
                to, where = on_plane(step)
                remote(send4.at[w, to], got4.at[w, plane], s4.at[w], r4.at[w], where).start()
            got4[w, plane] = send4[w, plane]

    def finish(w):
        with jax.named_scope(f"wait4#{w}"):
            rest = got4.at[w, pl.ds(0, PLANE - 1)]
            remote(rest, rest, s4.at[w], r4.at[w], partner).wait_recv()
        with jax.named_scope(f"finish#{w}"):
            gains = jnp.concatenate([gain_col[...]] * 3, axis=1)
            for g in range(2):
                v = got4[w, :, :, g * SPAN : (g + 1) * SPAN].astype(F32).reshape(WIDTH, SPAN)
                v = v - jnp.mean(v, axis=0, keepdims=True)
                v = v * lax.rsqrt(jnp.mean(v * v, axis=0, keepdims=True) + 1e-05)
                v = (v * gains).astype(BF16)
                out = lax.dot_general(v, weights[4], (((0,), (0,)), ((), ())), preferred_element_type=F32)
                out = out * gate[w * LANES + g * SPAN : w * LANES + (g + 1) * SPAN, :]
                for b in range(4):
                    for p, i in enumerate(STANDS):
                        flat[pl.ds(w * LANES + i * WI + 4 * g + b, WI, stride=WI), :] = out[
                            b * KB + p * WI : b * KB + (p + 1) * WI
                        ]
            out_hbm[:, w * WI : (w + 1) * WI, :] = flat[w * LANES : (w + 1) * LANES, :].reshape(KB, WI, WIDTH).astype(BF16)

    gather(0)
    gather(1)
    finish(0)
    gather(2)
    finish(1)
    finish(2)

    def sent(ref, sem):
        remote(ref, ref, sem, r4.at[0], partner).wait_send()

    with jax.named_scope("sent"):
        for w in range(WAVES):
            for a in range(2):
                sent(send1.at[a, w, pl.ds(0, DEPTH - 1)], s1.at[a, w])
                sent(send2.at[a, w, pl.ds(0, PLANE - 1)], s2.at[a, w])
            share(w).wait_send()
            sent(sums.at[w, pl.ds(0, 7 * PIECE), :], s3.at[w])
            sent(send4.at[w, pl.ds(0, PLANE - 1)], s4.at[w])


def body(pair_rows, in_gain, left_weight, right_weight, left_gate, right_gate, mid_gain, out_weight, out_gate):
    dma = pltpu.SemaphoreType.DMA
    vmem = pltpu.VMEM
    return pl.pallas_call(
        kernel,
        out_shape=pltpu.VMEM((KB, IB, WIDTH), BF16),
        in_specs=[pl.BlockSpec(memory_space=pltpu.MemorySpace.HBM)] * 9,
        out_specs=pl.BlockSpec(memory_space=vmem),
        scratch_shapes=[
            vmem((WAVES, KB, WI, WIDTH), BF16),
            vmem((1, WIDTH), F32),
            vmem((1, WIDTH), F32),
            vmem((6, WIDTH, WIDTH), BF16),
            vmem((4, WIDTH, WIDTH), F32),
            vmem((ROWS, WIDTH), F32),
            vmem((ROWS, WIDTH), BF16),
            vmem((4 * WIDTH, WIDTH), BF16),
            vmem((2, WAVES, DEPTH, PLANE, LANES), BF16),
            vmem((2, WAVES, DEPTH, PLANE, LANES), BF16),
            vmem((6, DEPTH * PLANE, 128), F32),
            vmem((2, 6, RES // 2, 128), F32),
            vmem((2, WAVES, PLANE, DEPTH, LANES), BF16),
            vmem((2, WAVES, PLANE, DEPTH, LANES), BF16),
            vmem((DEPTH, 2, WAVES, PIECE, RES), BF16),
            vmem((WAVES, SIDE, RES), BF16),
            vmem((WAVES, SIDE, RES), BF16),
            vmem((WAVES, DEPTH, PIECE, RES), BF16),
            vmem((WAVES, PLANE, 8, LANES), BF16),
            vmem((WAVES, PLANE, 8, LANES), BF16),
            vmem((ROWS, WIDTH), F32),
            vmem((WIDTH, WIDTH), F32),
            dma((WAVES,)), dma((2,)), dma((6,)),
            dma((2, WAVES)), dma((2, WAVES)),
            dma((2, WAVES)), dma((2, WAVES)),
            dma((WAVES,)), dma((WAVES,)),
            dma((WAVES,)), dma((WAVES,)),
            dma((WAVES,)), dma((WAVES,)),
        ],
        compiler_params=pltpu.CompilerParams(
            collective_id=0, has_side_effects=True, vmem_limit_bytes=60 * 2**20
        ),
        name="triangle",
    )(
        *(
            pltpu.with_memory_space_constraint(v, pltpu.MemorySpace.HBM)
            for v in (
                pair_rows, in_gain.reshape(1, WIDTH), left_weight, right_weight,
                left_gate, right_gate, mid_gain.reshape(1, WIDTH), out_weight, out_gate,
            )
        )
    )


def solution(mesh):
    placed = (P("north", "east", None), P(), P(), P(), P(), P(), P(), P(), P())
    return jax.shard_map(
        body, mesh=mesh, in_specs=placed, out_specs=P("north", "east", None), check_vma=False
    )
```

```python
import jax
import jax.numpy as jnp
from jax import lax
from jax.experimental import pallas as pl
from jax.experimental.pallas import tpu as pltpu
from jax.sharding import PartitionSpec as P

MESH = pl.DeviceIdType.MESH
F32, BF16 = jnp.float32, jnp.bfloat16

RES, WIDTH = 768, 128
NORTH, EAST, PLANE, DEPTH = 8, 32, 16, 8
KB, IB = RES // NORTH, RES // EAST
ROWS = KB * IB
WAVES, WI = 3, 8
LANES = WI * KB
SPAN = 4 * KB
PIECE = 2 * WI
SIDE = DEPTH * PIECE

STANDS = [y * 48 + c * 24 + w * WI for c in range(2) for w in range(WAVES) for y in range(2)]


ACROSS = sorted(
    ((dx, dy) for dx in range(4) for dy in range(4) if dx or dy),
    key=lambda step: -sum(min(d, 4 - d) for d in step),
)
ALONG = (3, 2, 1)


def turn(values, amount):
    amount = amount % SPAN
    return values if amount == 0 else pltpu.roll(values, amount, axis=1)


def regroup(parts):
    lane = lax.broadcasted_iota(jnp.int32, parts[0].shape, 1)
    out = []
    for b in range(4):
        row = turn(parts[0], -KB * b)
        for a in range(1, 4):
            row = jnp.where(lane >= KB * a, turn(parts[a], KB * (a - b)), row)
        out.append(row)
    return out


def nt(a, b):
    return lax.dot_general(a, b, (((1,), (1,)), ((), ())), preferred_element_type=F32)


def remote(src, dst, ssem, rsem, where):
    return pltpu.make_async_remote_copy(
        src_ref=src, dst_ref=dst, send_sem=ssem, recv_sem=rsem,
        device_id=where, device_id_type=MESH,
    )


def kernel(
    x_hbm, in_gain_hbm, lw_hbm, rw_hbm, lg_hbm, rg_hbm, mid_gain_hbm, ow_hbm, og_hbm, out_hbm,
    x, in_gain, mid_gain, weights, turned, flat, ready, wt, send1, got1, mid, lines, send2, got2,
    left, right, sums, got3, send4, got4, gate, gain_col,
    xs, gs, wsem, s1, r1, s2, r2, sf, rf, sn, rn, sq, rq, s3, r3, s4, r4,
):
    n = lax.axis_index("north")
    e = lax.axis_index("east")
    z, y, c = e // 4, lax.rem(e // 2, 2), lax.rem(e, 2)
    plane = n * 2 + y

    px, py = lax.rem(n, 4), (n // 4) * 2 + y

    def on_plane(step):
        x_to, y_to = lax.rem(px + step[0], 4), lax.rem(py + step[1], 4)
        n_to, y_to = (y_to // 2) * 4 + x_to, lax.rem(y_to, 2)
        return n_to * 2 + y_to, (n_to, (z * 2 + y_to) * 2 + c)

    def off(s):
        return lax.rem(z + (s + DEPTH), DEPTH)

    def on_line(to_z):
        return (n, (to_z * 2 + y) * 2 + c)

    partner = (n, (z * 2 + y) * 2 + 1 - c)

    fetch_x = [
        pltpu.make_async_copy(x_hbm.at[:, pl.ds(w * WI, WI), :], x.at[w], xs.at[w])
        for w in range(WAVES)
    ]
    fetch_w = [
        pltpu.make_async_copy(ref, weights.at[p], wsem.at[p])
        for p, ref in enumerate((lw_hbm, lg_hbm, rw_hbm, rg_hbm, ow_hbm, og_hbm))
    ]
    fetch_g = [
        pltpu.make_async_copy(in_gain_hbm, in_gain, gs.at[0]),
        pltpu.make_async_copy(mid_gain_hbm, mid_gain, gs.at[1]),
    ]
    for copy in [fetch_x[0], fetch_g[0], *fetch_w[:2], *fetch_x[1:], *fetch_w[2:], fetch_g[1]]:
        copy.start()

    with jax.named_scope("signal"):
        barrier = pltpu.get_barrier_semaphore()
        partners = [on_plane(step)[1] for step in ACROSS]
        partners += [on_line(off(s)) for s in (1, 2, 3, -1, -2, -3)] + [partner]
        for where in partners:
            pl.semaphore_signal(barrier, inc=1, device_id=where, device_id_type=MESH)

    def normalize(w):
        with jax.named_scope(f"norm#{w}"):
            fetch_x[w].wait()
            if w == 0:
                fetch_g[0].wait()
            v = x[w].astype(F32).reshape(LANES, WIDTH)
            v = v - jnp.mean(v, axis=-1, keepdims=True)
            v = v * lax.rsqrt(jnp.mean(v * v, axis=-1, keepdims=True) + 1e-05) * in_gain[...]
            flat[w * LANES : (w + 1) * LANES, :] = v
            for i in range(WI):
                line = [flat[pl.ds(w * LANES + k * WI + i, WI, stride=WI), :] for k in STANDS]
                at = (w * WI + i) * KB
                ready[at : at + KB, :] = jnp.concatenate(line, axis=0).astype(BF16)

    def orient(a):
        for p in range(2 * a, 2 * a + 2):
            fetch_w[p].wait()
            turned[p] = weights[p].astype(F32).T
            for to in range(DEPTH):
                at = p * WIDTH + to * PLANE
                wt[at : at + PLANE, :] = turned[p, pl.ds(to, PLANE, stride=DEPTH), :].astype(BF16)

    def project(a, w):
        with jax.named_scope(f"project#{a}{w}"):
            for g in range(2):
                rows = ready[w * LANES + g * SPAN : w * LANES + (g + 1) * SPAN, :]
                both = nt(wt[2 * a * WIDTH : 2 * (a + 1) * WIDTH, :], rows)
                both = both[:WIDTH] * jax.nn.sigmoid(both[WIDTH:])
                send1[a, w, :, :, g * SPAN : (g + 1) * SPAN] = both.reshape(DEPTH, PLANE, SPAN).astype(BF16)

    def along(a, w):
        for s in ALONG:
            for group, slot, to in ((off(s), s, off(s)), (off(-1 - s), 4 + s, off(-s))):
                remote(
                    send1.at[a, w, group], got1.at[a, w, slot], s1.at[a, w], r1.at[a, w], on_line(to)
                ).start()
        got1[a, w, 0] = send1[a, w, z]
        got1[a, w, 4] = send1[a, w, off(-1)]

    def across(a, w):
        with jax.named_scope(f"wait1#{a}{w}"):
            some = send1.at[a, w, pl.ds(0, 6)]
            remote(some, some, s1.at[a, w], r1.at[a, w], partner).wait_recv()
        with jax.named_scope(f"across#{a}{w}"):
            for t in range(6):
                for s in range(DEPTH):
                    mid[t, pl.ds(s, PLANE, stride=DEPTH), :] = got1[
                        a, w, s, :, t * 128 : (t + 1) * 128
                    ].astype(F32)
            for d in range(PLANE):
                for t in range(6):
                    send2[a, w, d, :, t * 128 : (t + 1) * 128] = mid[
                        t, d * DEPTH : (d + 1) * DEPTH, :
                    ].astype(BF16)
            for step in ACROSS:
                to, where = on_plane(step)
                remote(
                    send2.at[a, w, to], got2.at[a, w, plane], s2.at[a, w], r2.at[a, w], where
                ).start()
            got2[a, w, plane] = send2[a, w, plane]

    here = [(0, off(-s)) for s in range(4)] + [(1, off(s)) for s in range(4)]
    there = [(1, off(-1 - s)) for s in range(4)] + [(0, off(1 + s)) for s in range(4)]

    def share(w):
        for ch, line in here:
            mine = left.at[ch, line, c, w]
            to = on_line(off(1) if ch == 0 else off(-1))
            remote(mine, left.at[1 - ch, line, c, w], sn.at[w], rn.at[w], to).start()
        for ch, line in here:
            mine = left.at[ch, line, c, w]
            remote(mine, mine, sf.at[w], rf.at[w], partner).start()

    def hand_on(w):
        with jax.named_scope(f"hand#{w}"):
            remote(send1.at[0, w], send1.at[0, w], sn.at[w], rn.at[w], partner).wait_recv()
            for ch, line in there:
                mine = left.at[ch, line, c, w]
                remote(mine, mine, sq.at[w], rq.at[w], partner).start()

    def settle(a, w):
        with jax.named_scope(f"wait2#{a}{w}"):
            some = send2.at[a, w, pl.ds(0, PLANE - 1)]
            remote(some, some, s2.at[a, w], r2.at[a, w], partner).wait_recv()
        with jax.named_scope(f"settle#{a}{w}"):
            base, step = (w * PIECE, WAVES * PIECE) if a == 0 else (0, PIECE)
            for yy in range(2):
                for g in range(2):
                    for h in range(2):
                        parts = [
                            got2[a, w, (4 * h + q) * 2 + yy, :, g * SPAN : (g + 1) * SPAN].astype(F32)
                            for q in range(4)
                        ]
                        for b, row in enumerate(regroup(parts)):
                            at = pl.ds(base + yy * WI + 4 * g + b, DEPTH, stride=step)
                            for u in range(3):
                                lines[a, 3 * h + u, at, :] = row[:, u * 128 : (u + 1) * 128]
            for t in range(6):
                cols = slice(t * 128, (t + 1) * 128)
                if a == 0:
                    for s in range(DEPTH):
                        rows = slice(s * step + base, s * step + base + PIECE)
                        left[*here[s], c, w, :, cols] = lines[0, t, rows, :].astype(BF16)
                else:
                    right[w, :, cols] = lines[1, t, :SIDE, :].astype(BF16)
            if a == 0:
                share(w)

    orient(0)
    for w in range(WAVES):
        normalize(w)
        project(0, w)
        if w == 0:
            with jax.named_scope("barrier"):
                pl.semaphore_wait(barrier, PLANE + 6)
        along(0, w)
    orient(1)
    for w in range(WAVES):
        project(1, w)
        if w < 2:
            along(1, w)

    with jax.named_scope("gate"):
        fetch_w[4].wait()
        fetch_w[5].wait()
        fetch_g[1].wait()
        gain_col[...] = jnp.broadcast_to(mid_gain[...], (WIDTH, WIDTH)).T

        @pl.loop(0, ROWS // SPAN)
        def _(g):
            rows = pl.ds(pl.multiple_of(g * SPAN, SPAN), SPAN)
            gate[rows, :] = jax.nn.sigmoid(
                jnp.dot(ready[rows, :], weights[5], preferred_element_type=F32)
            )

    def multiply(w):
        if w == 0:
            with jax.named_scope("waitshare"):
                for ww in range(WAVES):
                    for ssem, rsem in ((sf, rf), (sq, rq)):
                        remote(send1.at[0, ww], send1.at[0, ww], ssem.at[ww], rsem.at[ww], partner).wait_recv()
        with jax.named_scope(f"mm#{w}"):
            for ch in range(2):
                rows = slice(ch * SIDE // 2, (ch + 1) * SIDE // 2)
                sums[w, rows, :] = (nt(right[w, rows, :], left[ch].reshape(RES, RES)) * RES ** (-0.5)).astype(BF16)
                group = off(-ch)
                for s in ALONG:
                    at = ch * SIDE // 2 + s * PIECE
                    remote(
                        sums.at[w, pl.ds(at, PIECE), :], got3.at[w, group], s3.at[w], r3.at[w],
                        on_line(off(-s if ch == 0 else s)),
                    ).start()
                got3[w, group] = sums[w, ch * SIDE // 2 : ch * SIDE // 2 + PIECE, :]

    across(0, 0)
    across(0, 1)
    settle(0, 0)
    across(0, 2)
    settle(0, 1)
    across(1, 0)
    settle(0, 2)
    along(1, 2)
    across(1, 1)
    hand_on(0)
    settle(1, 0)
    hand_on(1)
    settle(1, 1)
    hand_on(2)
    across(1, 2)
    multiply(0)
    multiply(1)
    settle(1, 2)
    multiply(2)

    def gather(w):
        with jax.named_scope(f"wait3#{w}"):
            some = sums.at[w, pl.ds(0, 6 * PIECE), :]
            remote(some, some, s3.at[w], r3.at[w], partner).wait_recv()
        with jax.named_scope(f"gather#{w}"):
            for d in range(DEPTH):
                for t in range(6):
                    mid[t, d * PIECE : (d + 1) * PIECE, :] = got3[
                        w, d, :, t * 128 : (t + 1) * 128
                    ].astype(F32)
            for yy in range(2):
                for g in range(2):
                    for h in range(2):
                        parts = [
                            jnp.concatenate(
                                [
                                    mid[3 * h + u, pl.ds(yy * WI + 4 * g + b, DEPTH, stride=PIECE), :]
                                    for u in range(3)
                                ],
                                axis=1,
                            )
                            for b in range(4)
                        ]
                        for q, row in enumerate(regroup(parts)):
                            send4[w, (4 * h + q) * 2 + yy, :, g * SPAN : (g + 1) * SPAN] = row.astype(BF16)
            for step in ACROSS:
                to, where = on_plane(step)
                remote(send4.at[w, to], got4.at[w, plane], s4.at[w], r4.at[w], where).start()
            got4[w, plane] = send4[w, plane]

    def finish(w):
        with jax.named_scope(f"wait4#{w}"):
            rest = got4.at[w, pl.ds(0, PLANE - 1)]
            remote(rest, rest, s4.at[w], r4.at[w], partner).wait_recv()
        with jax.named_scope(f"finish#{w}"):
            gains = jnp.concatenate([gain_col[...]] * 3, axis=1)
            for g in range(2):
                v = got4[w, :, :, g * SPAN : (g + 1) * SPAN].astype(F32).reshape(WIDTH, SPAN)
                v = v - jnp.mean(v, axis=0, keepdims=True)
                v = v * lax.rsqrt(jnp.mean(v * v, axis=0, keepdims=True) + 1e-05)
                v = (v * gains).astype(BF16)
                out = lax.dot_general(v, weights[4], (((0,), (0,)), ((), ())), preferred_element_type=F32)
                out = out * gate[w * LANES + g * SPAN : w * LANES + (g + 1) * SPAN, :]
                for b in range(4):
                    for p, i in enumerate(STANDS):
                        flat[pl.ds(w * LANES + i * WI + 4 * g + b, WI, stride=WI), :] = out[
                            b * KB + p * WI : b * KB + (p + 1) * WI
                        ]
            out_hbm[:, w * WI : (w + 1) * WI, :] = flat[w * LANES : (w + 1) * LANES, :].reshape(KB, WI, WIDTH).astype(BF16)

    gather(0)
    gather(1)
    gather(2)
    finish(0)
    finish(1)
    finish(2)

    def sent(ref, sem):
        remote(ref, ref, sem, r4.at[0], partner).wait_send()

    with jax.named_scope("sent"):
        for w in range(WAVES):
            for a in range(2):
                sent(send1.at[a, w, pl.ds(0, 6)], s1.at[a, w])
                sent(send2.at[a, w, pl.ds(0, PLANE - 1)], s2.at[a, w])
            for sem in (sf, sn, sq):
                sent(send1.at[0, w], sem.at[w])
            sent(sums.at[w, pl.ds(0, 6 * PIECE), :], s3.at[w])
            sent(send4.at[w, pl.ds(0, PLANE - 1)], s4.at[w])


def body(pair_rows, in_gain, left_weight, right_weight, left_gate, right_gate, mid_gain, out_weight, out_gate):
    dma = pltpu.SemaphoreType.DMA
    vmem = pltpu.VMEM
    return pl.pallas_call(
        kernel,
        out_shape=pltpu.VMEM((KB, IB, WIDTH), BF16),
        in_specs=[pl.BlockSpec(memory_space=pltpu.MemorySpace.HBM)] * 9,
        out_specs=pl.BlockSpec(memory_space=vmem),
        scratch_shapes=[
            vmem((WAVES, KB, WI, WIDTH), BF16),
            vmem((1, WIDTH), F32),
            vmem((1, WIDTH), F32),
            vmem((6, WIDTH, WIDTH), BF16),
            vmem((4, WIDTH, WIDTH), F32),
            vmem((ROWS, WIDTH), F32),
            vmem((ROWS, WIDTH), BF16),
            vmem((4 * WIDTH, WIDTH), BF16),
            vmem((2, WAVES, DEPTH, PLANE, LANES), BF16),
            vmem((2, WAVES, DEPTH, PLANE, LANES), BF16),
            vmem((6, DEPTH * PLANE, 128), F32),
            vmem((2, 6, RES // 2, 128), F32),
            vmem((2, WAVES, PLANE, DEPTH, LANES), BF16),
            vmem((2, WAVES, PLANE, DEPTH, LANES), BF16),
            vmem((2, DEPTH, 2, WAVES, PIECE, RES), BF16),
            vmem((WAVES, SIDE, RES), BF16),
            vmem((WAVES, SIDE, RES), BF16),
            vmem((WAVES, DEPTH, PIECE, RES), BF16),
            vmem((WAVES, PLANE, 8, LANES), BF16),
            vmem((WAVES, PLANE, 8, LANES), BF16),
            vmem((ROWS, WIDTH), F32),
            vmem((WIDTH, WIDTH), F32),
            dma((WAVES,)), dma((2,)), dma((6,)),
            dma((2, WAVES)), dma((2, WAVES)),
            dma((2, WAVES)), dma((2, WAVES)),
            dma((WAVES,)), dma((WAVES,)),
            dma((WAVES,)), dma((WAVES,)),
            dma((WAVES,)), dma((WAVES,)),
            dma((WAVES,)), dma((WAVES,)),
            dma((WAVES,)), dma((WAVES,)),
        ],
        compiler_params=pltpu.CompilerParams(
            collective_id=0, has_side_effects=True, vmem_limit_bytes=60 * 2**20
        ),
        name="triangle",
    )(
        *(
            pltpu.with_memory_space_constraint(v, pltpu.MemorySpace.HBM)
            for v in (
                pair_rows, in_gain.reshape(1, WIDTH), left_weight, right_weight,
                left_gate, right_gate, mid_gain.reshape(1, WIDTH), out_weight, out_gate,
            )
        )
    )


def solution(mesh):
    placed = (P("north", "east", None), P(), P(), P(), P(), P(), P(), P(), P())
    return jax.shard_map(
        body, mesh=mesh, in_specs=placed, out_specs=P("north", "east", None), check_vma=False
    )
```

```python
import jax
import jax.numpy as jnp
from jax import lax
from jax.experimental import pallas as pl
from jax.experimental.pallas import tpu as pltpu
from jax.sharding import PartitionSpec as P

MESH = pl.DeviceIdType.MESH
F32, BF16 = jnp.float32, jnp.bfloat16

RES, WIDTH = 768, 128
NORTH, EAST, PLANE, DEPTH = 8, 32, 16, 8
KB, IB = RES // NORTH, RES // EAST
ROWS = KB * IB
WAVES, WI = 3, 8
LANES = WI * KB
SPAN = 4 * KB
PIECE = 2 * WI
SIDE = DEPTH * PIECE

STANDS = [y * 48 + c * 24 + w * WI for c in range(2) for w in range(WAVES) for y in range(2)]


ACROSS = sorted(
    ((dx, dy) for dx in range(4) for dy in range(4) if dx or dy),
    key=lambda step: -sum(min(d, 4 - d) for d in step),
)
ALONG = (3, 2, 1)


def turn(values, amount):
    amount = amount % SPAN
    return values if amount == 0 else pltpu.roll(values, amount, axis=1)


def regroup(parts):
    lane = lax.broadcasted_iota(jnp.int32, parts[0].shape, 1)
    out = []
    for b in range(4):
        row = turn(parts[0], -KB * b)
        for a in range(1, 4):
            row = jnp.where(lane >= KB * a, turn(parts[a], KB * (a - b)), row)
        out.append(row)
    return out


def nt(a, b):
    return lax.dot_general(a, b, (((1,), (1,)), ((), ())), preferred_element_type=F32)


def remote(src, dst, ssem, rsem, where):
    return pltpu.make_async_remote_copy(
        src_ref=src, dst_ref=dst, send_sem=ssem, recv_sem=rsem,
        device_id=where, device_id_type=MESH,
    )


def kernel(
    x_hbm, in_gain_hbm, lw_hbm, rw_hbm, lg_hbm, rg_hbm, mid_gain_hbm, ow_hbm, og_hbm, out_hbm,
    x, in_gain, mid_gain, weights, turned, flat, ready, wt, send1, got1, mid, lines, send2, got2,
    left, right, sums, got3, send4, got4, gate, gain_col,
    xs, gs, wsem, s1, r1, s2, r2, sf, rf, sn, rn, sq, rq, s3, r3, s4, r4,
):
    n = lax.axis_index("north")
    e = lax.axis_index("east")
    z, y, c = e // 4, lax.rem(e // 2, 2), lax.rem(e, 2)
    plane = n * 2 + y

    px, py = lax.rem(n, 4), (n // 4) * 2 + y

    def on_plane(step):
        x_to, y_to = lax.rem(px + step[0], 4), lax.rem(py + step[1], 4)
        n_to, y_to = (y_to // 2) * 4 + x_to, lax.rem(y_to, 2)
        return n_to * 2 + y_to, (n_to, (z * 2 + y_to) * 2 + c)

    def off(s):
        return lax.rem(z + (s + DEPTH), DEPTH)

    def on_line(to_z):
        return (n, (to_z * 2 + y) * 2 + c)

    partner = (n, (z * 2 + y) * 2 + 1 - c)

    fetch_x = [
        pltpu.make_async_copy(x_hbm.at[:, pl.ds(w * WI, WI), :], x.at[w], xs.at[w])
        for w in range(WAVES)
    ]
    fetch_w = [
        pltpu.make_async_copy(ref, weights.at[p], wsem.at[p])
        for p, ref in enumerate((lw_hbm, lg_hbm, rw_hbm, rg_hbm, ow_hbm, og_hbm))
    ]
    fetch_g = [
        pltpu.make_async_copy(in_gain_hbm, in_gain, gs.at[0]),
        pltpu.make_async_copy(mid_gain_hbm, mid_gain, gs.at[1]),
    ]
    for copy in [fetch_x[0], fetch_g[0], *fetch_w[:2], *fetch_x[1:], *fetch_w[2:], fetch_g[1]]:
        copy.start()

    with jax.named_scope("signal"):
        barrier = pltpu.get_barrier_semaphore()
        partners = [on_plane(step)[1] for step in ACROSS]
        partners += [on_line(off(s)) for s in (1, 2, 3, -1, -2, -3)] + [partner]
        for where in partners:
            pl.semaphore_signal(barrier, inc=1, device_id=where, device_id_type=MESH)

    def normalize(w):
        with jax.named_scope(f"norm#{w}"):
            fetch_x[w].wait()
            if w == 0:
                fetch_g[0].wait()
            v = x[w].astype(F32).reshape(LANES, WIDTH)
            v = v - jnp.mean(v, axis=-1, keepdims=True)
            v = v * lax.rsqrt(jnp.mean(v * v, axis=-1, keepdims=True) + 1e-05) * in_gain[...]
            flat[w * LANES : (w + 1) * LANES, :] = v
            for i in range(WI):
                line = [flat[pl.ds(w * LANES + k * WI + i, WI, stride=WI), :] for k in STANDS]
                at = (w * WI + i) * KB
                ready[at : at + KB, :] = jnp.concatenate(line, axis=0).astype(BF16)

    def orient(a):
        for p in range(2 * a, 2 * a + 2):
            fetch_w[p].wait()
            turned[p] = weights[p].astype(F32).T
            for to in range(DEPTH):
                at = p * WIDTH + to * PLANE
                wt[at : at + PLANE, :] = turned[p, pl.ds(to, PLANE, stride=DEPTH), :].astype(BF16)

    def project(a, w):
        with jax.named_scope(f"project#{a}{w}"):
            for g in range(2):
                rows = ready[w * LANES + g * SPAN : w * LANES + (g + 1) * SPAN, :]
                both = nt(wt[2 * a * WIDTH : 2 * (a + 1) * WIDTH, :], rows)
                both = both[:WIDTH] * jax.nn.sigmoid(both[WIDTH:])
                send1[a, w, :, :, g * SPAN : (g + 1) * SPAN] = both.reshape(DEPTH, PLANE, SPAN).astype(BF16)

    def along(a, w):
        for s in ALONG:
            for group, slot, to in ((off(s), s, off(s)), (off(-1 - s), 4 + s, off(-s))):
                remote(
                    send1.at[a, w, group], got1.at[a, w, slot], s1.at[a, w], r1.at[a, w], on_line(to)
                ).start()
        got1[a, w, 0] = send1[a, w, z]
        got1[a, w, 4] = send1[a, w, off(-1)]

    def across(a, w):
        with jax.named_scope(f"wait1#{a}{w}"):
            some = send1.at[a, w, pl.ds(0, 6)]
            remote(some, some, s1.at[a, w], r1.at[a, w], partner).wait_recv()
        with jax.named_scope(f"across#{a}{w}"):
            for t in range(6):
                for s in range(DEPTH):
                    mid[t, pl.ds(s, PLANE, stride=DEPTH), :] = got1[
                        a, w, s, :, t * 128 : (t + 1) * 128
                    ].astype(F32)
            for d in range(PLANE):
                for t in range(6):
                    send2[a, w, d, :, t * 128 : (t + 1) * 128] = mid[
                        t, d * DEPTH : (d + 1) * DEPTH, :
                    ].astype(BF16)
            for step in ACROSS:
                to, where = on_plane(step)
                remote(
                    send2.at[a, w, to], got2.at[a, w, plane], s2.at[a, w], r2.at[a, w], where
                ).start()
            got2[a, w, plane] = send2[a, w, plane]

    here = [(0, off(-s)) for s in range(4)] + [(1, off(s)) for s in range(4)]
    there = [(1, off(-1 - s)) for s in range(4)] + [(0, off(1 + s)) for s in range(4)]

    def share(w):
        for s in (0, 4, 1, 5, 2, 6, 3, 7):
            ch, line = here[s]
            mine = left.at[ch, line, c, w]
            to = on_line(off(1) if ch == 0 else off(-1))
            remote(mine, left.at[1 - ch, line, c, w], sn.at[w], rn.at[w], to).start()
        for ch, line in here:
            mine = left.at[ch, line, c, w]
            remote(mine, mine, sf.at[w], rf.at[w], partner).start()

    def hand_on(w):
        with jax.named_scope(f"hand#{w}"):
            remote(send1.at[0, w], send1.at[0, w], sn.at[w], rn.at[w], partner).wait_recv()
            for ch, line in there:
                mine = left.at[ch, line, c, w]
                remote(mine, mine, sq.at[w], rq.at[w], partner).start()

    def settle(a, w):
        with jax.named_scope(f"wait2#{a}{w}"):
            some = send2.at[a, w, pl.ds(0, PLANE - 1)]
            remote(some, some, s2.at[a, w], r2.at[a, w], partner).wait_recv()
        with jax.named_scope(f"settle#{a}{w}"):
            base, step = (w * PIECE, WAVES * PIECE) if a == 0 else (0, PIECE)
            for yy in range(2):
                for g in range(2):
                    for h in range(2):
                        parts = [
                            got2[a, w, (4 * h + q) * 2 + yy, :, g * SPAN : (g + 1) * SPAN].astype(F32)
                            for q in range(4)
                        ]
                        for b, row in enumerate(regroup(parts)):
                            at = pl.ds(base + yy * WI + 4 * g + b, DEPTH, stride=step)
                            for u in range(3):
                                lines[a, 3 * h + u, at, :] = row[:, u * 128 : (u + 1) * 128]
            for t in range(6):
                cols = slice(t * 128, (t + 1) * 128)
                if a == 0:
                    for s in range(DEPTH):
                        rows = slice(s * step + base, s * step + base + PIECE)
                        left[*here[s], c, w, :, cols] = lines[0, t, rows, :].astype(BF16)
                else:
                    right[w, :, cols] = lines[1, t, :SIDE, :].astype(BF16)
            if a == 0:
                share(w)

    orient(0)
    for w in range(WAVES):
        normalize(w)
        project(0, w)
        if w == 0:
            with jax.named_scope("barrier"):
                pl.semaphore_wait(barrier, PLANE + 6)
        along(0, w)
    orient(1)
    for w in range(WAVES):
        project(1, w)
        if w < 2:
            along(1, w)

    with jax.named_scope("gate"):
        fetch_w[4].wait()
        fetch_w[5].wait()
        fetch_g[1].wait()
        gain_col[...] = jnp.broadcast_to(mid_gain[...], (WIDTH, WIDTH)).T

        @pl.loop(0, ROWS // SPAN)
        def _(g):
            rows = pl.ds(pl.multiple_of(g * SPAN, SPAN), SPAN)
            gate[rows, :] = jax.nn.sigmoid(
                jnp.dot(ready[rows, :], weights[5], preferred_element_type=F32)
            )

    def multiply(w):
        if w == 0:
            with jax.named_scope("waitshare"):
                for ww in range(WAVES):
                    for ssem, rsem in ((sf, rf), (sq, rq)):
                        remote(send1.at[0, ww], send1.at[0, ww], ssem.at[ww], rsem.at[ww], partner).wait_recv()
        with jax.named_scope(f"mm#{w}"):
            for ch in range(2):
                rows = slice(ch * SIDE // 2, (ch + 1) * SIDE // 2)
                sums[w, rows, :] = (nt(right[w, rows, :], left[ch].reshape(RES, RES)) * RES ** (-0.5)).astype(BF16)
                group = off(-ch)
                for s in ALONG:
                    at = ch * SIDE // 2 + s * PIECE
                    remote(
                        sums.at[w, pl.ds(at, PIECE), :], got3.at[w, group], s3.at[w], r3.at[w],
                        on_line(off(-s if ch == 0 else s)),
                    ).start()
                got3[w, group] = sums[w, ch * SIDE // 2 : ch * SIDE // 2 + PIECE, :]

    across(0, 0)
    across(0, 1)
    settle(0, 0)
    across(0, 2)
    settle(0, 1)
    across(1, 0)
    settle(0, 2)
    along(1, 2)
    across(1, 1)
    hand_on(0)
    settle(1, 0)
    hand_on(1)
    settle(1, 1)
    hand_on(2)
    across(1, 2)
    multiply(0)
    multiply(1)
    settle(1, 2)
    multiply(2)

    def gather(w):
        with jax.named_scope(f"wait3#{w}"):
            some = sums.at[w, pl.ds(0, 6 * PIECE), :]
            remote(some, some, s3.at[w], r3.at[w], partner).wait_recv()
        with jax.named_scope(f"gather#{w}"):
            for d in range(DEPTH):
                for t in range(6):
                    mid[t, d * PIECE : (d + 1) * PIECE, :] = got3[
                        w, d, :, t * 128 : (t + 1) * 128
                    ].astype(F32)
            for yy in range(2):
                for g in range(2):
                    for h in range(2):
                        parts = [
                            jnp.concatenate(
                                [
                                    mid[3 * h + u, pl.ds(yy * WI + 4 * g + b, DEPTH, stride=PIECE), :]
                                    for u in range(3)
                                ],
                                axis=1,
                            )
                            for b in range(4)
                        ]
                        for q, row in enumerate(regroup(parts)):
                            send4[w, (4 * h + q) * 2 + yy, :, g * SPAN : (g + 1) * SPAN] = row.astype(BF16)
            for step in ACROSS:
                to, where = on_plane(step)
                remote(send4.at[w, to], got4.at[w, plane], s4.at[w], r4.at[w], where).start()
            got4[w, plane] = send4[w, plane]

    def finish(w):
        with jax.named_scope(f"wait4#{w}"):
            rest = got4.at[w, pl.ds(0, PLANE - 1)]
            remote(rest, rest, s4.at[w], r4.at[w], partner).wait_recv()
        with jax.named_scope(f"finish#{w}"):
            gains = jnp.concatenate([gain_col[...]] * 3, axis=1)
            for g in range(2):
                v = got4[w, :, :, g * SPAN : (g + 1) * SPAN].astype(F32).reshape(WIDTH, SPAN)
                v = v - jnp.mean(v, axis=0, keepdims=True)
                v = v * lax.rsqrt(jnp.mean(v * v, axis=0, keepdims=True) + 1e-05)
                v = (v * gains).astype(BF16)
                out = lax.dot_general(v, weights[4], (((0,), (0,)), ((), ())), preferred_element_type=F32)
                out = out * gate[w * LANES + g * SPAN : w * LANES + (g + 1) * SPAN, :]
                for b in range(4):
                    for p, i in enumerate(STANDS):
                        flat[pl.ds(w * LANES + i * WI + 4 * g + b, WI, stride=WI), :] = out[
                            b * KB + p * WI : b * KB + (p + 1) * WI
                        ]
            out_hbm[:, w * WI : (w + 1) * WI, :] = flat[w * LANES : (w + 1) * LANES, :].reshape(KB, WI, WIDTH).astype(BF16)

    gather(0)
    gather(1)
    gather(2)
    finish(0)
    finish(1)
    finish(2)

    def sent(ref, sem):
        remote(ref, ref, sem, r4.at[0], partner).wait_send()

    with jax.named_scope("sent"):
        for w in range(WAVES):
            for a in range(2):
                sent(send1.at[a, w, pl.ds(0, 6)], s1.at[a, w])
                sent(send2.at[a, w, pl.ds(0, PLANE - 1)], s2.at[a, w])
            for sem in (sf, sn, sq):
                sent(send1.at[0, w], sem.at[w])
            sent(sums.at[w, pl.ds(0, 6 * PIECE), :], s3.at[w])
            sent(send4.at[w, pl.ds(0, PLANE - 1)], s4.at[w])


def body(pair_rows, in_gain, left_weight, right_weight, left_gate, right_gate, mid_gain, out_weight, out_gate):
    dma = pltpu.SemaphoreType.DMA
    vmem = pltpu.VMEM
    return pl.pallas_call(
        kernel,
        out_shape=pltpu.VMEM((KB, IB, WIDTH), BF16),
        in_specs=[pl.BlockSpec(memory_space=pltpu.MemorySpace.HBM)] * 9,
        out_specs=pl.BlockSpec(memory_space=vmem),
        scratch_shapes=[
            vmem((WAVES, KB, WI, WIDTH), BF16),
            vmem((1, WIDTH), F32),
            vmem((1, WIDTH), F32),
            vmem((6, WIDTH, WIDTH), BF16),
            vmem((4, WIDTH, WIDTH), F32),
            vmem((ROWS, WIDTH), F32),
            vmem((ROWS, WIDTH), BF16),
            vmem((4 * WIDTH, WIDTH), BF16),
            vmem((2, WAVES, DEPTH, PLANE, LANES), BF16),
            vmem((2, WAVES, DEPTH, PLANE, LANES), BF16),
            vmem((6, DEPTH * PLANE, 128), F32),
            vmem((2, 6, RES // 2, 128), F32),
            vmem((2, WAVES, PLANE, DEPTH, LANES), BF16),
            vmem((2, WAVES, PLANE, DEPTH, LANES), BF16),
            vmem((2, DEPTH, 2, WAVES, PIECE, RES), BF16),
            vmem((WAVES, SIDE, RES), BF16),
            vmem((WAVES, SIDE, RES), BF16),
            vmem((WAVES, DEPTH, PIECE, RES), BF16),
            vmem((WAVES, PLANE, 8, LANES), BF16),
            vmem((WAVES, PLANE, 8, LANES), BF16),
            vmem((ROWS, WIDTH), F32),
            vmem((WIDTH, WIDTH), F32),
            dma((WAVES,)), dma((2,)), dma((6,)),
            dma((2, WAVES)), dma((2, WAVES)),
            dma((2, WAVES)), dma((2, WAVES)),
            dma((WAVES,)), dma((WAVES,)),
            dma((WAVES,)), dma((WAVES,)),
            dma((WAVES,)), dma((WAVES,)),
            dma((WAVES,)), dma((WAVES,)),
            dma((WAVES,)), dma((WAVES,)),
        ],
        compiler_params=pltpu.CompilerParams(
            collective_id=0, has_side_effects=True, vmem_limit_bytes=60 * 2**20
        ),
        name="triangle",
    )(
        *(
            pltpu.with_memory_space_constraint(v, pltpu.MemorySpace.HBM)
            for v in (
                pair_rows, in_gain.reshape(1, WIDTH), left_weight, right_weight,
                left_gate, right_gate, mid_gain.reshape(1, WIDTH), out_weight, out_gate,
            )
        )
    )


def solution(mesh):
    placed = (P("north", "east", None), P(), P(), P(), P(), P(), P(), P(), P())
    return jax.shard_map(
        body, mesh=mesh, in_specs=placed, out_specs=P("north", "east", None), check_vma=False
    )
```

```python
import jax
import jax.numpy as jnp
from jax import lax
from jax.experimental import pallas as pl
from jax.experimental.pallas import tpu as pltpu
from jax.sharding import PartitionSpec as P

MESH = pl.DeviceIdType.MESH
F32, BF16 = jnp.float32, jnp.bfloat16

RES, WIDTH = 768, 128
NORTH, EAST, PLANE, DEPTH = 8, 32, 16, 8
KB, IB = RES // NORTH, RES // EAST
ROWS = KB * IB
WAVES, WI = 3, 8
LANES = WI * KB
SPAN = 4 * KB
PIECE = 2 * WI
SIDE = DEPTH * PIECE

STANDS = [y * 48 + c * 24 + w * WI for c in range(2) for w in range(WAVES) for y in range(2)]


ACROSS = sorted(
    ((dx, dy) for dx in range(4) for dy in range(4) if dx or dy),
    key=lambda step: -sum(min(d, 4 - d) for d in step),
)
ALONG = (3, 2, 1)


def turn(values, amount):
    amount = amount % SPAN
    return values if amount == 0 else pltpu.roll(values, amount, axis=1)


def regroup(parts):
    lane = lax.broadcasted_iota(jnp.int32, parts[0].shape, 1)
    out = []
    for b in range(4):
        row = turn(parts[0], -KB * b)
        for a in range(1, 4):
            row = jnp.where(lane >= KB * a, turn(parts[a], KB * (a - b)), row)
        out.append(row)
    return out


def nt(a, b):
    return lax.dot_general(a, b, (((1,), (1,)), ((), ())), preferred_element_type=F32)


def remote(src, dst, ssem, rsem, where):
    return pltpu.make_async_remote_copy(
        src_ref=src, dst_ref=dst, send_sem=ssem, recv_sem=rsem,
        device_id=where, device_id_type=MESH,
    )


def kernel(
    x_hbm, in_gain_hbm, lw_hbm, rw_hbm, lg_hbm, rg_hbm, mid_gain_hbm, ow_hbm, og_hbm, out_hbm,
    x, in_gain, mid_gain, weights, turned, flat, ready, wt, send1, got1, mid, lines, send2, got2,
    left, right, sums, got3, send4, got4, gate, gain_col,
    xs, gs, wsem, s1, r1, s2, r2, sf, rf, sn, rn, sq, rq, s3, r3, s4, r4,
):
    n = lax.axis_index("north")
    e = lax.axis_index("east")
    z, y, c = e // 4, lax.rem(e // 2, 2), lax.rem(e, 2)
    plane = n * 2 + y

    px, py = lax.rem(n, 4), (n // 4) * 2 + y

    def on_plane(step):
        x_to, y_to = lax.rem(px + step[0], 4), lax.rem(py + step[1], 4)
        n_to, y_to = (y_to // 2) * 4 + x_to, lax.rem(y_to, 2)
        return n_to * 2 + y_to, (n_to, (z * 2 + y_to) * 2 + c)

    def off(s):
        return lax.rem(z + (s + DEPTH), DEPTH)

    def on_line(to_z):
        return (n, (to_z * 2 + y) * 2 + c)

    partner = (n, (z * 2 + y) * 2 + 1 - c)

    fetch_x = [
        pltpu.make_async_copy(x_hbm.at[:, pl.ds(w * WI, WI), :], x.at[w], xs.at[w])
        for w in range(WAVES)
    ]
    fetch_w = [
        pltpu.make_async_copy(ref, weights.at[p], wsem.at[p])
        for p, ref in enumerate((lw_hbm, lg_hbm, rw_hbm, rg_hbm, ow_hbm, og_hbm))
    ]
    fetch_g = [
        pltpu.make_async_copy(in_gain_hbm, in_gain, gs.at[0]),
        pltpu.make_async_copy(mid_gain_hbm, mid_gain, gs.at[1]),
    ]
    for copy in [fetch_x[0], fetch_g[0], *fetch_w[:2], *fetch_x[1:], *fetch_w[2:], fetch_g[1]]:
        copy.start()

    with jax.named_scope("signal"):
        barrier = pltpu.get_barrier_semaphore()
        partners = [on_plane(step)[1] for step in ACROSS]
        partners += [on_line(off(s)) for s in (1, 2, 3, -1, -2, -3)] + [partner]
        for where in partners:
            pl.semaphore_signal(barrier, inc=1, device_id=where, device_id_type=MESH)

    def normalize(w):
        with jax.named_scope(f"norm#{w}"):
            fetch_x[w].wait()
            if w == 0:
                fetch_g[0].wait()
            v = x[w].astype(F32).reshape(LANES, WIDTH)
            v = v - jnp.mean(v, axis=-1, keepdims=True)
            v = v * lax.rsqrt(jnp.mean(v * v, axis=-1, keepdims=True) + 1e-05) * in_gain[...]
            flat[w * LANES : (w + 1) * LANES, :] = v
            for i in range(WI):
                line = [flat[pl.ds(w * LANES + k * WI + i, WI, stride=WI), :] for k in STANDS]
                at = (w * WI + i) * KB
                ready[at : at + KB, :] = jnp.concatenate(line, axis=0).astype(BF16)

    def orient(a):
        for p in range(2 * a, 2 * a + 2):
            fetch_w[p].wait()
            turned[p] = weights[p].astype(F32).T
            for to in range(DEPTH):
                at = p * WIDTH + to * PLANE
                wt[at : at + PLANE, :] = turned[p, pl.ds(to, PLANE, stride=DEPTH), :].astype(BF16)

    def project(a, w):
        with jax.named_scope(f"project#{a}{w}"):
            for g in range(2):
                rows = ready[w * LANES + g * SPAN : w * LANES + (g + 1) * SPAN, :]
                both = nt(wt[2 * a * WIDTH : 2 * (a + 1) * WIDTH, :], rows)
                both = both[:WIDTH] * jax.nn.sigmoid(both[WIDTH:])
                send1[a, w, :, :, g * SPAN : (g + 1) * SPAN] = both.reshape(DEPTH, PLANE, SPAN).astype(BF16)

    def along(a, w):
        for s in ALONG:
            for group, slot, to in ((off(s), s, off(s)), (off(-1 - s), 4 + s, off(-s))):
                remote(
                    send1.at[a, w, group], got1.at[a, w, slot], s1.at[a, w], r1.at[a, w], on_line(to)
                ).start()
        got1[a, w, 0] = send1[a, w, z]
        got1[a, w, 4] = send1[a, w, off(-1)]

    def across(a, w):
        with jax.named_scope(f"wait1#{a}{w}"):
            some = send1.at[a, w, pl.ds(0, 6)]
            remote(some, some, s1.at[a, w], r1.at[a, w], partner).wait_recv()
        with jax.named_scope(f"across#{a}{w}"):
            for t in range(6):
                for s in range(DEPTH):
                    mid[t, pl.ds(s, PLANE, stride=DEPTH), :] = got1[
                        a, w, s, :, t * 128 : (t + 1) * 128
                    ].astype(F32)
            for d in range(PLANE):
                for t in range(6):
                    send2[a, w, d, :, t * 128 : (t + 1) * 128] = mid[
                        t, d * DEPTH : (d + 1) * DEPTH, :
                    ].astype(BF16)
            for step in ACROSS:
                to, where = on_plane(step)
                remote(
                    send2.at[a, w, to], got2.at[a, w, plane], s2.at[a, w], r2.at[a, w], where
                ).start()
            got2[a, w, plane] = send2[a, w, plane]

    here = [(0, off(-s)) for s in range(4)] + [(1, off(s)) for s in range(4)]
    there = [(1, off(-1 - s)) for s in range(4)] + [(0, off(1 + s)) for s in range(4)]

    def share(w):
        for s in (0, 4, 1, 5, 2, 6, 3, 7):
            ch, line = here[s]
            mine = left.at[ch, line, c, w]
            to = on_line(off(1) if ch == 0 else off(-1))
            remote(mine, left.at[1 - ch, line, c, w], sn.at[w], rn.at[w], to).start()
        for ch, line in here:
            mine = left.at[ch, line, c, w]
            remote(mine, mine, sf.at[w], rf.at[w], partner).start()

    def hand_on(w):
        with jax.named_scope(f"hand#{w}"):
            remote(send1.at[0, w], send1.at[0, w], sn.at[w], rn.at[w], partner).wait_recv()
            for ch, line in there:
                mine = left.at[ch, line, c, w]
                remote(mine, mine, sq.at[w], rq.at[w], partner).start()

    def settle(a, w):
        with jax.named_scope(f"wait2#{a}{w}"):
            some = send2.at[a, w, pl.ds(0, PLANE - 1)]
            remote(some, some, s2.at[a, w], r2.at[a, w], partner).wait_recv()
        with jax.named_scope(f"settle#{a}{w}"):
            base, step = (w * PIECE, WAVES * PIECE) if a == 0 else (0, PIECE)
            for yy in range(2):
                for g in range(2):
                    for h in range(2):
                        parts = [
                            got2[a, w, (4 * h + q) * 2 + yy, :, g * SPAN : (g + 1) * SPAN].astype(F32)
                            for q in range(4)
                        ]
                        for b, row in enumerate(regroup(parts)):
                            at = pl.ds(base + yy * WI + 4 * g + b, DEPTH, stride=step)
                            for u in range(3):
                                lines[a, 3 * h + u, at, :] = row[:, u * 128 : (u + 1) * 128]
            for t in range(6):
                cols = slice(t * 128, (t + 1) * 128)
                if a == 0:
                    for s in range(DEPTH):
                        rows = slice(s * step + base, s * step + base + PIECE)
                        left[*here[s], c, w, :, cols] = lines[0, t, rows, :].astype(BF16)
                else:
                    right[w, :, cols] = lines[1, t, :SIDE, :].astype(BF16)
            if a == 0:
                share(w)

    orient(0)
    for w in range(WAVES):
        normalize(w)
        project(0, w)
        if w == 0:
            with jax.named_scope("barrier"):
                pl.semaphore_wait(barrier, PLANE + 6)
        along(0, w)
    orient(1)
    for w in range(WAVES):
        project(1, w)
        if w < 2:
            along(1, w)

    with jax.named_scope("gate"):
        fetch_w[4].wait()
        fetch_w[5].wait()
        fetch_g[1].wait()
        gain_col[...] = jnp.broadcast_to(mid_gain[...], (WIDTH, WIDTH)).T

        @pl.loop(0, ROWS // SPAN)
        def _(g):
            rows = pl.ds(pl.multiple_of(g * SPAN, SPAN), SPAN)
            gate[rows, :] = jax.nn.sigmoid(
                jnp.dot(ready[rows, :], weights[5], preferred_element_type=F32)
            )

    def multiply(w):
        if w == 0:
            with jax.named_scope("waitshare"):
                for ww in range(WAVES):
                    for ssem, rsem in ((sf, rf), (sq, rq)):
                        remote(send1.at[0, ww], send1.at[0, ww], ssem.at[ww], rsem.at[ww], partner).wait_recv()
        with jax.named_scope(f"mm#{w}"):
            for ch in range(2):
                rows = slice(ch * SIDE // 2, (ch + 1) * SIDE // 2)
                sums[w, rows, :] = (nt(right[w, rows, :], left[ch].reshape(RES, RES)) * RES ** (-0.5)).astype(BF16)
                group = off(-ch)
                for s in ALONG:
                    at = ch * SIDE // 2 + s * PIECE
                    remote(
                        sums.at[w, pl.ds(at, PIECE), :], got3.at[w, group], s3.at[w], r3.at[w],
                        on_line(off(-s if ch == 0 else s)),
                    ).start()
                got3[w, group] = sums[w, ch * SIDE // 2 : ch * SIDE // 2 + PIECE, :]

    across(0, 0)
    across(0, 1)
    settle(0, 0)
    across(0, 2)
    settle(0, 1)
    across(1, 0)
    settle(0, 2)
    along(1, 2)
    hand_on(0)
    across(1, 1)
    hand_on(1)
    settle(1, 0)
    hand_on(2)
    settle(1, 1)
    across(1, 2)
    multiply(0)
    multiply(1)
    settle(1, 2)
    multiply(2)

    def gather(w):
        with jax.named_scope(f"wait3#{w}"):
            some = sums.at[w, pl.ds(0, 6 * PIECE), :]
            remote(some, some, s3.at[w], r3.at[w], partner).wait_recv()
        with jax.named_scope(f"gather#{w}"):
            for d in range(DEPTH):
                for t in range(6):
                    mid[t, d * PIECE : (d + 1) * PIECE, :] = got3[
                        w, d, :, t * 128 : (t + 1) * 128
                    ].astype(F32)
            for yy in range(2):
                for g in range(2):
                    for h in range(2):
                        parts = [
                            jnp.concatenate(
                                [
                                    mid[3 * h + u, pl.ds(yy * WI + 4 * g + b, DEPTH, stride=PIECE), :]
                                    for u in range(3)
                                ],
                                axis=1,
                            )
                            for b in range(4)
                        ]
                        for q, row in enumerate(regroup(parts)):
                            send4[w, (4 * h + q) * 2 + yy, :, g * SPAN : (g + 1) * SPAN] = row.astype(BF16)
            for step in ACROSS:
                to, where = on_plane(step)
                remote(send4.at[w, to], got4.at[w, plane], s4.at[w], r4.at[w], where).start()
            got4[w, plane] = send4[w, plane]

    def finish(w):
        with jax.named_scope(f"wait4#{w}"):
            rest = got4.at[w, pl.ds(0, PLANE - 1)]
            remote(rest, rest, s4.at[w], r4.at[w], partner).wait_recv()
        with jax.named_scope(f"finish#{w}"):
            gains = jnp.concatenate([gain_col[...]] * 3, axis=1)
            for g in range(2):
                v = got4[w, :, :, g * SPAN : (g + 1) * SPAN].astype(F32).reshape(WIDTH, SPAN)
                v = v - jnp.mean(v, axis=0, keepdims=True)
                v = v * lax.rsqrt(jnp.mean(v * v, axis=0, keepdims=True) + 1e-05)
                v = (v * gains).astype(BF16)
                out = lax.dot_general(v, weights[4], (((0,), (0,)), ((), ())), preferred_element_type=F32)
                out = out * gate[w * LANES + g * SPAN : w * LANES + (g + 1) * SPAN, :]
                for b in range(4):
                    for p, i in enumerate(STANDS):
                        flat[pl.ds(w * LANES + i * WI + 4 * g + b, WI, stride=WI), :] = out[
                            b * KB + p * WI : b * KB + (p + 1) * WI
                        ]
            out_hbm[:, w * WI : (w + 1) * WI, :] = flat[w * LANES : (w + 1) * LANES, :].reshape(KB, WI, WIDTH).astype(BF16)

    gather(0)
    gather(1)
    gather(2)
    finish(0)
    finish(1)
    finish(2)

    def sent(ref, sem):
        remote(ref, ref, sem, r4.at[0], partner).wait_send()

    with jax.named_scope("sent"):
        for w in range(WAVES):
            for a in range(2):
                sent(send1.at[a, w, pl.ds(0, 6)], s1.at[a, w])
                sent(send2.at[a, w, pl.ds(0, PLANE - 1)], s2.at[a, w])
            for sem in (sf, sn, sq):
                sent(send1.at[0, w], sem.at[w])
            sent(sums.at[w, pl.ds(0, 6 * PIECE), :], s3.at[w])
            sent(send4.at[w, pl.ds(0, PLANE - 1)], s4.at[w])


def body(pair_rows, in_gain, left_weight, right_weight, left_gate, right_gate, mid_gain, out_weight, out_gate):
    dma = pltpu.SemaphoreType.DMA
    vmem = pltpu.VMEM
    return pl.pallas_call(
        kernel,
        out_shape=pltpu.VMEM((KB, IB, WIDTH), BF16),
        in_specs=[pl.BlockSpec(memory_space=pltpu.MemorySpace.HBM)] * 9,
        out_specs=pl.BlockSpec(memory_space=vmem),
        scratch_shapes=[
            vmem((WAVES, KB, WI, WIDTH), BF16),
            vmem((1, WIDTH), F32),
            vmem((1, WIDTH), F32),
            vmem((6, WIDTH, WIDTH), BF16),
            vmem((4, WIDTH, WIDTH), F32),
            vmem((ROWS, WIDTH), F32),
            vmem((ROWS, WIDTH), BF16),
            vmem((4 * WIDTH, WIDTH), BF16),
            vmem((2, WAVES, DEPTH, PLANE, LANES), BF16),
            vmem((2, WAVES, DEPTH, PLANE, LANES), BF16),
            vmem((6, DEPTH * PLANE, 128), F32),
            vmem((2, 6, RES // 2, 128), F32),
            vmem((2, WAVES, PLANE, DEPTH, LANES), BF16),
            vmem((2, WAVES, PLANE, DEPTH, LANES), BF16),
            vmem((2, DEPTH, 2, WAVES, PIECE, RES), BF16),
            vmem((WAVES, SIDE, RES), BF16),
            vmem((WAVES, SIDE, RES), BF16),
            vmem((WAVES, DEPTH, PIECE, RES), BF16),
            vmem((WAVES, PLANE, 8, LANES), BF16),
            vmem((WAVES, PLANE, 8, LANES), BF16),
            vmem((ROWS, WIDTH), F32),
            vmem((WIDTH, WIDTH), F32),
            dma((WAVES,)), dma((2,)), dma((6,)),
            dma((2, WAVES)), dma((2, WAVES)),
            dma((2, WAVES)), dma((2, WAVES)),
            dma((WAVES,)), dma((WAVES,)),
            dma((WAVES,)), dma((WAVES,)),
            dma((WAVES,)), dma((WAVES,)),
            dma((WAVES,)), dma((WAVES,)),
            dma((WAVES,)), dma((WAVES,)),
        ],
        compiler_params=pltpu.CompilerParams(
            collective_id=0, has_side_effects=True, vmem_limit_bytes=60 * 2**20
        ),
        name="triangle",
    )(
        *(
            pltpu.with_memory_space_constraint(v, pltpu.MemorySpace.HBM)
            for v in (
                pair_rows, in_gain.reshape(1, WIDTH), left_weight, right_weight,
                left_gate, right_gate, mid_gain.reshape(1, WIDTH), out_weight, out_gate,
            )
        )
    )


def solution(mesh):
    placed = (P("north", "east", None), P(), P(), P(), P(), P(), P(), P(), P())
    return jax.shard_map(
        body, mesh=mesh, in_specs=placed, out_specs=P("north", "east", None), check_vma=False
    )
```
